256 devices in a mesh: vol: 2 (over z), row: 128 (over y, x, core).
Axes of the slice: x: 8, y: 8, z: 2, core: 2. Of those that a mesh axis runs over, the one named last changes fastest.
The devices are a block of a 8x8x16 slice.
Arguments:
- volume: float32 [6, 2048, 2048], P('vol', 'row'), parts along dimension 0, may hold values from 0.25 to 2
- psf_spectra: bfloat16 [2, 3, 2048, 2048], P(None, None, 'row'), may hold values from -3.5 to 3.5
- background: float32 [2048, 2048], P('row'), may hold values from 1 to 4
- measured: float32 [4096, 2048], P(('vol', 'row')), parts along dimension 0, may hold values from 0.5 to 4
Outputs:
- new_volume: float32 [6, 2048, 2048], P('vol', 'row'), parts along dimension 0
- projection: float32 [4096, 2048], P(('vol', 'row')), parts along dimension 0
The draws below stay inside these ranges and needn't reach their ends.
There are 2 independent parts, one for each index of `vol`. The reference program is written for one: setup_inputs(seed, part) draws one part's arguments, and reference() takes and returns one part's arrays. A program takes and returns all parts, laid end to end along the dimension named above; an argument that names none is the same for every part. Nothing has to cross between parts.
All inputs are finite; a program needn't handle non-finite values.
Results may differ from the reference program's by a relative error of at most 0.0003.
Values sent between devices are 32-bit elements; how exact they have to be, the bound alone decides.
A program may use at most 64 MiB of HBM per device.

```python
import math
import jax
import jax.numpy as jnp
from jax import lax

SENSOR = 2048
DEPTHS = 3


def shard_levels(own_key, dims, cuts, least, high):
    loudness = 1.0
    for dim, blocks in cuts:
        heights = jax.random.uniform(jax.random.fold_in(jax.random.fold_in(own_key, 6), dim), (blocks,), jnp.float32, least / len(cuts), high / len(cuts))
        loudness = loudness * jnp.repeat(jnp.exp(heights), dims[dim] // blocks).reshape((-1,) + (1,) * (len(dims) - 1 - dim))
    return loudness


def centred(own_key, extent, deviation, most, cuts=(), kind=jnp.bfloat16):
    array = jax.random.normal(own_key, extent, jnp.float32) * deviation
    if len(cuts) > 0:
        array = shard_levels(own_key, extent, cuts, -0.22, 0.18) * array
    return jnp.clip(array, min=-most, max=most).astype(kind)


def setup_inputs(seed: int = 0, part: int = 0) -> dict:
    seeds = jax.random.split(jax.random.key(seed), 5)
    own_keys = jax.random.split(jax.random.fold_in(seeds[4], part), 5)
    volume = jnp.clip(jnp.exp(math.log(2.0) - 2.0794415 * jax.random.uniform(own_keys[0], (DEPTHS, SENSOR, SENSOR), jnp.float32) ** shard_levels(own_keys[0], (DEPTHS, SENSOR, SENSOR), ((1, 128),), -0.2, 0.2)), 0.25, 2.0)
    psf_spectra = centred(seeds[1], (2, DEPTHS, SENSOR, SENSOR), DEPTHS ** -0.5, 3.5, ((2, 128),))
    background = jnp.clip(jnp.exp(math.log(4.0) - 1.3862944 * jax.random.uniform(seeds[2], (SENSOR, SENSOR), jnp.float32) ** shard_levels(seeds[2], (SENSOR, SENSOR), ((0, 128),), -0.2, 0.2)), 1.0, 4.0)
    measured = jnp.clip(jnp.exp(math.log(4.0) - 2.0794415 * jax.random.uniform(own_keys[3], (SENSOR, SENSOR), jnp.float32) ** shard_levels(own_keys[3], (SENSOR, SENSOR), ((0, 128),), -0.2, 0.2)), 0.5, 4.0)
    return {"volume": volume, "psf_spectra": psf_spectra, "background": background, "measured": measured}


FLOOR = 0.5


def reference(volume, psf_spectra, background, measured):
    response = psf_spectra[0].astype(jnp.float32) + 1j * psf_spectra[1].astype(jnp.float32)
    response = jnp.swapaxes(response, 1, 2)

    def project_slice(carry, pieces):
        layer, kernel = pieces
        return carry + jnp.fft.fft2(layer) * kernel, 0

    initial = jnp.zeros(volume.shape[1:], response.dtype)
    summed, unused = lax.scan(project_slice, initial, (volume, response))
    projection = jnp.real(jnp.fft.ifft2(summed)).astype(jnp.float32)
    quotient = measured / jnp.maximum(projection + background, FLOOR)
    quotient_spec = jnp.fft.fft2(quotient)

    def correct_slice(pieces):
        layer, kernel = pieces
        back = jnp.real(jnp.fft.ifft2(quotient_spec * jnp.conj(kernel))).astype(jnp.float32)
        return layer * back

    new_volume = lax.map(correct_slice, (volume, response))
    return new_volume, projection
```

```python
import functools
import math

import jax
import jax.numpy as jnp
import ml_dtypes
import numpy as np
from jax import lax
from jax.experimental import pallas as pl
from jax.experimental.pallas import tpu as pltpu
from jax.sharding import PartitionSpec as P

FLOOR = 0.5
F32 = jnp.float32
BF16 = jnp.bfloat16
NN = (((1,), (0,)), ((), ()))
NT = (((1,), (1,)), ((), ()))


def split_np(table):
    hi = table.astype(np.float32).astype(ml_dtypes.bfloat16)
    lo = (table - hi.astype(np.float64)).astype(np.float32).astype(ml_dtypes.bfloat16)
    return np.stack([hi, lo])


def tables(n, q):
    length = n * q
    half = q // 2
    big = np.exp(-2j * np.pi * np.outer(np.arange(n), np.arange(n)) / n)
    small = np.exp(-2j * np.pi * np.outer(np.arange(q), np.arange(q)) / q)
    big_stack = np.block([[big.real, -big.imag], [big.imag, big.real]])
    spread = np.kron(small, np.eye(q))
    ycols = np.concatenate([spread.real, spread.imag], axis=0)
    mixed = np.einsum("xk,ij->ixkj", small, np.eye(half)).reshape(half * q, q * half)
    xmix = np.block([[mixed.real, mixed.imag], [-mixed.imag, mixed.real]])
    twist = np.exp(-2j * np.pi * np.outer(np.arange(q), np.arange(n)) / length)
    ytw = np.repeat(twist, q, axis=0)
    xtw = np.tile(twist.T, (1, half))
    pair = lambda z: np.stack([z.real, z.imag]).astype(np.float32)
    return (
        split_np(big_stack),
        split_np(ycols),
        split_np(np.ascontiguousarray(ycols.T)),
        split_np(xmix),
        pair(ytw),
        pair(ytw.T),
        pair(xtw),
    )


def split(value):
    hi = value.astype(BF16)
    return hi, (value - hi.astype(F32)).astype(BF16)


def dot3(left, right, dims):
    mul = functools.partial(lax.dot_general, dimension_numbers=dims, preferred_element_type=F32)
    return mul(left[0], right[0]) + mul(left[0], right[1]) + mul(left[1], right[0])


def kernel(
    n, q, slices,
    vol_ref, psf_ref, back_ref, meas_ref,
    big_ref, ycol_ref, yrow_ref, xmix_ref, ytw_ref, ytwt_ref, xtw_ref,
    out_ref, proj_ref,
    send_buf, recv_buf, resp, send_sems, recv_sems,
):
    half = q // 2
    lanes = half * q
    scale = 1.0 / (n * q * n * q)
    me = lax.axis_index("row")
    vol_id = lax.axis_index("vol")

    def peer(step):
        return lax.rem(me + step, n)

    barrier = pltpu.get_barrier_semaphore()

    @pl.loop(1, n)
    def _(step):
        pl.semaphore_signal(
            barrier, inc=1, device_id=(vol_id, peer(step)), device_id_type=pl.DeviceIdType.MESH
        )

    def table(ref):
        return ref[0], ref[1]

    def copy_to(slot, dst):
        return pltpu.make_async_remote_copy(
            src_ref=send_buf.at[slot, dst],
            dst_ref=recv_buf.at[slot, me],
            send_sem=send_sems.at[slot],
            recv_sem=recv_sems.at[slot],
            device_id=(vol_id, dst),
            device_id_type=pl.DeviceIdType.MESH,
        )

    def start(slot):
        @pl.loop(1, n)
        def _(step):
            copy_to(slot, peer(step)).start()

        recv_buf[slot, me] = send_buf[slot, me]

    def whole(slot):
        return pltpu.make_async_remote_copy(
            src_ref=send_buf.at[slot, pl.ds(0, n - 1)],
            dst_ref=recv_buf.at[slot, pl.ds(0, n - 1)],
            send_sem=send_sems.at[slot],
            recv_sem=recv_sems.at[slot],
            device_id=(vol_id, peer(1)),
            device_id_type=pl.DeviceIdType.MESH,
        )

    def put(slot, stacked, order):
        for place, part in enumerate(order):
            for h in range(2):
                send_buf[slot, :, part * 2 + h, :] = stacked[
                    place * n : (place + 1) * n, h * lanes : (h + 1) * lanes
                ]

    def get(slot, order):
        rows = []
        for part in order:
            rows.append(
                jnp.concatenate([recv_buf[slot, :, part * 2 + h, :] for h in range(2)], axis=1)
            )
        return jnp.concatenate(rows, axis=0)

    def stack_rows(read):
        return jnp.concatenate([read(a) for a in range(q)], axis=0)

    def y_forward(field, slot):
        mixed = dot3(table(ycol_ref), split(field), NN)
        re, im = mixed[: q * q], mixed[q * q :]
        wr, wi = ytw_ref[0], ytw_ref[1]
        turned = jnp.concatenate([re * wr - im * wi, re * wi + im * wr], axis=1)
        put(slot, dot3(table(big_ref), split(turned), NT), (0, 1))

    def x_forward(slot):
        got = dot3(table(big_ref), split(get(slot, (0, 1))), NN)
        wr, wi = xtw_ref[0], xtw_ref[1]
        rows = []
        for h in range(2):
            re = got[:n, h * lanes : (h + 1) * lanes]
            im = got[n:, h * lanes : (h + 1) * lanes]
            rows.append(jnp.concatenate([re * wr - im * wi, re * wi + im * wr], axis=1))
        spec = dot3(split(jnp.concatenate(rows, axis=0)), table(xmix_ref), NN)
        return spec[:, :lanes], spec[:, lanes:]

    def x_inverse(re, im, slot):
        mixed = dot3(split(jnp.concatenate([re, im], axis=1)), table(xmix_ref), NT)
        wr, wi = xtw_ref[0], xtw_ref[1]
        real_cols, imag_cols = [], []
        for h in range(2):
            re = mixed[h * n : (h + 1) * n, :lanes]
            im = mixed[h * n : (h + 1) * n, lanes:]
            real_cols.append(re * wr + im * wi)
            imag_cols.append(im * wr - re * wi)
        swapped = jnp.concatenate(
            [jnp.concatenate(imag_cols, axis=1), jnp.concatenate(real_cols, axis=1)], axis=0
        )
        put(slot, dot3(table(big_ref), split(swapped), NN), (1, 0))

    def y_inverse(slot):
        got = dot3(table(big_ref), split(get(slot, (1, 0))), NN)
        im, re = got[:n], got[n:]
        wr, wi = ytwt_ref[0], ytwt_ref[1]
        turned = jnp.concatenate([re * wr + im * wi, im * wr - re * wi], axis=1)
        return dot3(table(yrow_ref), split(turned), NT) * scale

    for d in range(slices):
        y_forward(stack_rows(lambda a: vol_ref[d, :, a * n : (a + 1) * n]), d)
        if d == 0:
            pl.semaphore_wait(barrier, n - 1)
        start(d)

    for part in range(2):
        for d in range(slices):
            for h in range(2):
                block = jnp.concatenate(
                    [
                        psf_ref[part, d, :, k * n : (k + 1) * n].astype(F32)[
                            h * half : (h + 1) * half
                        ]
                        for k in range(q)
                    ],
                    axis=0,
                )
                resp[part, d, h * n : (h + 1) * n, :] = block.T

    sum_re = sum_im = None
    for d in range(slices):
        whole(d).wait_recv()
        re, im = x_forward(d)
        rr, ri = resp[0, d], resp[1, d]
        pr, pi = re * rr - im * ri, re * ri + im * rr
        sum_re = pr if d == 0 else sum_re + pr
        sum_im = pi if d == 0 else sum_im + pi
    x_inverse(sum_re, sum_im, slices)
    start(slices)
    whole(slices).wait_recv()
    projection = y_inverse(slices)
    quotient = []
    for a in range(q):
        cols = slice(a * n, (a + 1) * n)
        piece = projection[a * q : (a + 1) * q]
        proj_ref[:, cols] = piece
        quotient.append(meas_ref[:, cols] / jnp.maximum(piece + back_ref[:, cols], FLOOR))
    y_forward(jnp.concatenate(quotient, axis=0), slices + 1)
    start(slices + 1)
    whole(slices + 1).wait_recv()
    qr, qi = x_forward(slices + 1)
    for d in range(slices):
        rr, ri = resp[0, d], resp[1, d]
        x_inverse(qr * rr + qi * ri, qi * rr - qr * ri, slices + 2 + d)
        start(slices + 2 + d)
    for d in range(slices):
        whole(slices + 2 + d).wait_recv()
        correction = y_inverse(slices + 2 + d)
        for a in range(q):
            cols = slice(a * n, (a + 1) * n)
            out_ref[d, :, cols] = vol_ref[d, :, cols] * correction[a * q : (a + 1) * q]
    for slot in range(2 * slices + 2):
        whole(slot).wait_send()


def shards(volume, psf_spectra, background, measured):
    n = lax.axis_size("row")
    slices, q, length = volume.shape
    slots = 2 * slices + 2
    consts = tables(n, q)
    in_vmem = pl.BlockSpec(memory_space=pltpu.VMEM)
    return pl.pallas_call(
        functools.partial(kernel, n, q, slices),
        out_shape=(
            jax.ShapeDtypeStruct(volume.shape, F32),
            jax.ShapeDtypeStruct(measured.shape, F32),
        ),
        in_specs=[in_vmem] * (4 + len(consts)),
        out_specs=(in_vmem, in_vmem),
        scratch_shapes=[
            pltpu.VMEM((slots, n, 4, q * q // 2), F32),
            pltpu.VMEM((slots, n, 4, q * q // 2), F32),
            pltpu.VMEM((2, slices, 2 * n, q * q // 2), F32),
            pltpu.SemaphoreType.DMA((slots,)),
            pltpu.SemaphoreType.DMA((slots,)),
        ],
        compiler_params=pltpu.CompilerParams(
            collective_id=0, has_side_effects=True, vmem_limit_bytes=60 * 1024 * 1024
        ),
    )(volume, psf_spectra, background, measured, *consts)


def solution(mesh):
    in_specs = (
        P("vol", "row", None),
        P(None, None, "row", None),
        P("row", None),
        P(("vol", "row"), None),
    )
    out_specs = (P("vol", "row", None), P(("vol", "row"), None))
    return jax.shard_map(shards, mesh=mesh, in_specs=in_specs, out_specs=out_specs, check_vma=False)
```

```python
import functools

import jax
import jax.numpy as jnp
import ml_dtypes
import numpy as np
from jax import lax
from jax.experimental import pallas as pl
from jax.experimental.pallas import tpu as pltpu
from jax.sharding import PartitionSpec as P

FLOOR = 0.5
F32 = jnp.float32
BF16 = jnp.bfloat16
NN = (((1,), (0,)), ((), ()))
NT = (((1,), (1,)), ((), ()))
GROUPS = ((0, 1), (2,))


def split_np(table):
    hi = table.astype(np.float32).astype(ml_dtypes.bfloat16)
    lo = (table - hi.astype(np.float64)).astype(np.float32).astype(ml_dtypes.bfloat16)
    return np.stack([hi, lo])


def tables(n, q):
    length = n * q
    half = q // 2
    lanes = half * q
    big = np.exp(-2j * np.pi * np.outer(np.arange(n), np.arange(n)) / n)
    small = np.exp(-2j * np.pi * np.outer(np.arange(q), np.arange(q)) / q)
    big_stack = np.block([[big.real, -big.imag], [big.imag, big.real]])
    spread = np.kron(small[: half + 1], np.eye(q))
    ycols = np.concatenate([spread.real, spread.imag], axis=0)
    yrows = np.zeros((q * q, 2, 2 * lanes))
    yrows[:, 0, : (half + 1) * q] = spread.real.T
    yrows[:, 1, : (half + 1) * q] = spread.imag.T
    mixed = np.einsum("xk,ij->ixkj", small, np.eye(half)).reshape(lanes, q * half)
    xmix = np.block([[mixed.real, mixed.imag], [-mixed.imag, mixed.real]])
    twist = np.exp(-2j * np.pi * np.outer(np.arange(q), np.arange(n)) / length)
    ytw = np.repeat(twist[: half + 1], q, axis=0)
    ytwt = np.zeros((n, 2 * lanes), complex)
    ytwt[:, : (half + 1) * q] = ytw.T
    xtw = np.tile(twist.T, (1, half))
    pair = lambda z: np.stack([z.real, z.imag]).astype(np.float32)
    return (
        split_np(ycols),
        pair(ytw),
        split_np(big_stack),
        pair(xtw),
        split_np(xmix),
        pair(ytwt),
        split_np(yrows.reshape(q * q, 4 * lanes)),
    )


def split(value):
    hi = value.astype(BF16)
    return hi, (value - hi.astype(F32)).astype(BF16)


def dot(left, right, dims):
    return lax.dot_general(left, right, dimension_numbers=dims, preferred_element_type=F32)


def dot3(left, right, dims):
    return dot(left[0], right[0], dims) + dot(left[0], right[1], dims) + dot(left[1], right[0], dims)


def kernel(n, q, slices, counts, *refs):
    ins, refs = refs[:11], refs[11:]
    out_ref, proj_ref = refs[:2]
    held, refs = refs[2:13], refs[13:]
    messages = len(counts)
    sends, recvs = refs[:messages], refs[messages : 2 * messages]
    (
        own_half, main_send, main_recv, row_send, row_self, row_recv, resp, resp_mix, spec, spec_mix, total,
        in_sems, send_sems, recv_sems, psf_sems, row_sems, late_sem,
    ) = refs[2 * messages :]
    vol_ref, psf_ref, back_ref, meas_ref, ycol_ref, ytw_ref, big_ref, xtw_ref, xmix_ref, ytwt_ref, yrow_ref = held
    order = (1, 0, 4, 5, 6, 7, 8, 9, 10, 2, 3)
    parts = len(GROUPS)
    half = q // 2
    middle = n // 2
    scale = 1.0 / (n * q * n * q)
    me = lax.axis_index("row")
    vol_id = lax.axis_index("vol")
    row_iota = lax.broadcasted_iota(jnp.int32, (n, n), 0)
    lane_iota = lax.broadcasted_iota(jnp.int32, (n, n), 1)

    def fetch(i):
        return pltpu.make_async_copy(ins[i], held[i], in_sems.at[i])

    for i in order:
        fetch(i).start()

    def device(dst):
        return (vol_id, dst)

    def tell(sem, dst):
        pl.semaphore_signal(sem, inc=1, device_id=device(dst), device_id_type=pl.DeviceIdType.MESH)

    barrier = pltpu.get_barrier_semaphore()

    def peer(step):
        return jnp.bitwise_and(me + step, n - 1)

    @pl.when(me < 2)
    def _():
        tell(barrier, 1 - me)

    @pl.when(me >= 2)
    def _():
        @pl.loop(1, n)
        def _(step):
            tell(barrier, peer(step))

    def copy_to(m, dst):
        return pltpu.make_async_remote_copy(
            src_ref=sends[m].at[dst],
            dst_ref=recvs[m].at[me],
            send_sem=send_sems.at[m],
            recv_sem=recv_sems.at[m],
            device_id=device(dst),
            device_id_type=pl.DeviceIdType.MESH,
        )

    def start(m):
        @pl.loop(1, n, unroll=8)
        def _(step):
            copy_to(m, peer(step)).start()

        recvs[m][me] = sends[m][me]

    def whole(m):
        return pltpu.make_async_remote_copy(
            src_ref=sends[m].at[pl.ds(0, n - 1)],
            dst_ref=recvs[m].at[pl.ds(0, n - 1)],
            send_sem=send_sems.at[m],
            recv_sem=recv_sems.at[m],
            device_id=device(peer(1)),
            device_id_type=pl.DeviceIdType.MESH,
        )

    def main_copy(dst):
        return pltpu.make_async_remote_copy(
            src_ref=main_send,
            dst_ref=main_recv,
            send_sem=psf_sems.at[0],
            recv_sem=psf_sems.at[1],
            device_id=device(dst),
            device_id_type=pl.DeviceIdType.MESH,
        )

    def row_copy(dst):
        return pltpu.make_async_remote_copy(
            src_ref=row_send,
            dst_ref=row_recv,
            send_sem=row_sems.at[0],
            recv_sem=row_sems.at[1],
            device_id=device(dst),
            device_id_type=pl.DeviceIdType.MESH,
        )

    def table(ref):
        return ref[0], ref[1]

    def y_forward(field, m, at):
        mixed = dot3(table(ycol_ref), split(field), NN)
        kept = (half + 1) * q
        re, im = mixed[:kept], mixed[kept:]
        wr, wi = ytw_ref[0], ytw_ref[1]
        turned = jnp.concatenate([re * wr - im * wi, re * wi + im * wr], axis=1)
        both = jnp.concatenate([turned[: half * q], turned[half * q :], turned[q : half * q]], axis=0)
        got = dot3(table(big_ref), split(both), NT)
        lanes = half * q
        re = jnp.concatenate([got[:middle, lanes:], got[middle:n, :lanes]], axis=0)
        im = jnp.concatenate([got[n : n + middle, lanes:], got[n + middle :, :lanes]], axis=0)
        im = jnp.where((row_iota == middle) & (lane_iota < q), got[0:1, :lanes], im)
        sends[m][:, 2 * at, :] = re
        sends[m][:, 2 * at + 1, :] = im

    def x_forward(re, im):
        got = dot3(table(big_ref), split(jnp.concatenate([re, im], axis=0)), NN)
        re, im = got[:n], got[n:]
        wr, wi = xtw_ref[0], xtw_ref[1]
        turned = jnp.concatenate([re * wr - im * wi, re * wi + im * wr], axis=1)
        out = dot3(split(turned), table(xmix_ref), NN)
        return out[:, :n], out[:, n:]

    def x_forward_conj(fields):
        re_sum = im_sum = jnp.zeros((n, n), F32)
        for d, (re, im) in enumerate(fields):
            mine = (lane_iota >= d * q) & (lane_iota < (d + 1) * q)
            if d:
                re, im = pltpu.roll(re, d * q, 1), pltpu.roll(im, d * q, 1)
            re_sum = jnp.where(mine, re, re_sum)
            im_sum = jnp.where(mine, -im, im_sum)
        return x_forward(re_sum, im_sum)

    def x_inverse(re, im, m, at):
        mixed = dot3(split(jnp.concatenate([re, im], axis=1)), table(xmix_ref), NT)
        wr, wi = xtw_ref[0], xtw_ref[1]
        re, im = mixed[:, :n], mixed[:, n:]
        swapped = jnp.concatenate([im * wr - re * wi, re * wr + im * wi], axis=0)
        got = dot3(table(big_ref), split(swapped), NN)
        sends[m][:, 2 * at, :] = got[n:]
        sends[m][:, 2 * at + 1, :] = got[:n]

    def y_inverse(m, at):
        re, im = recvs[m][:, 2 * at, :], recvs[m][:, 2 * at + 1, :]
        first = lane_iota < q
        upper = first & (row_iota < middle)
        zero_row = first & (row_iota == 0)
        mid_row = first & (row_iota == middle)
        re_low = jnp.where(upper, 0.0, re)
        re_low = jnp.where(mid_row, 0.5 * re, re_low)
        re_low = jnp.where(zero_row, 0.5 * im[middle : middle + 1], re_low)
        im_low = jnp.where(upper | mid_row, 0.0, im)
        re_high, im_high = jnp.where(upper, re, 0.0), jnp.where(upper, im, 0.0)
        swapped = jnp.concatenate(
            [
                jnp.concatenate([im_low, im_high], axis=1),
                jnp.concatenate([re_low, re_high], axis=1),
            ],
            axis=0,
        )
        got = dot3(table(big_ref), split(swapped), NN)
        im, re = got[:n], got[n:]
        wr, wi = ytwt_ref[0], ytwt_ref[1]
        turned = jnp.concatenate([re * wr + im * wi, im * wr - re * wi], axis=1)
        return dot3(table(yrow_ref), split(turned), NT) * (2.0 * scale)

    fetch(1).wait()
    reverse = jnp.where((row_iota + lane_iota == n) | (row_iota + lane_iota == 0), 1.0, 0.0).astype(BF16)
    same_block = row_iota // half == lane_iota // half
    slot_sum = row_iota % half + lane_iota % half
    slot_flip = jnp.where(same_block & ((slot_sum == half) | (slot_sum == 0)), 1.0, 0.0).astype(BF16)

    def blocks(field, backwards):
        places = range(q - 1, -1, -1) if backwards else range(q)
        return jnp.concatenate([field[:, k * n : (k + 1) * n] for k in places], axis=0)

    def mend(field):
        return jnp.where(row_iota == 0, pltpu.roll(field, half, 1), field)

    sub_iota = lax.broadcasted_iota(jnp.int32, (half, n * q), 0)
    rows = []
    for part in range(2):
        for d in range(slices):
            at = part * slices + d
            sign = 0.5 if part == 0 else -0.5
            both = psf_ref[part, d].astype(F32)
            low, high = both[:half], both[half:]
            rows.append(low[0:1])
            own = jnp.where((sub_iota == 0) & (me < middle), high, low)
            own_half[at] = 0.5 * blocks(own, False).T
            turned = dot(reverse, blocks(high, True).astype(BF16), NT)
            turned = dot(turned.astype(BF16), slot_flip, NN)
            main_send[at] = sign * mend(turned)
    packed = jnp.concatenate(rows + [jnp.zeros((half - 2 * slices, n * q), F32)], axis=0)
    turned = mend(dot(reverse, blocks(packed, True).astype(BF16), NT))
    mine = jnp.where(lane_iota % half < slices, 0.5, -0.5) * turned
    row_self[...] = mine
    row_send[...] = jnp.where(me == 0, mine + 0.5 * blocks(packed, False).T, mine)

    @pl.when(me >= 2)
    def _():
        pl.semaphore_wait(barrier, n - 3)

    @pl.when(me < 2)
    def _():
        pl.semaphore_wait(barrier, n - 1)

        @pl.when(me == 1)
        def _():
            @pl.loop(2, n)
            def _(dst):
                tell(late_sem, dst)

    @pl.when(me < n - 2)
    def _():
        main_copy(n - 1 - me).start()

    @pl.when(me == 0)
    def _():
        row_copy(middle).start()

    @pl.when((me > 0) & (me < middle))
    def _():
        row_copy(n - me).start()

    for i in (0, 4, 5, 6):
        fetch(i).wait()
    for m, group in enumerate(GROUPS):
        for at, d in enumerate(group):
            y_forward(
                jnp.concatenate([vol_ref[d, :, a * n : (a + 1) * n] for a in range(q)], axis=0), m, at
            )

        @pl.when(me >= 2)
        def _():
            @pl.loop(1, n - 2, unroll=5)
            def _(step):
                place = me + step
                copy_to(m, jnp.where(place >= n, place - (n - 2), place)).start()

        @pl.when(me < 2)
        def _():
            @pl.loop(1, n, unroll=8)
            def _(step):
                copy_to(m, peer(step)).start()

        recvs[m][me] = sends[m][me]

    @pl.when(me >= 2)
    def _():
        pl.semaphore_wait(late_sem, 1)
        for dst in range(2):
            for m in range(parts):
                copy_to(m, dst).start()

    @pl.when(me >= n - 2)
    def _():
        main_copy(n - 1 - me).start()

    main_copy(n - 1 - me).wait_recv()
    slot_zero = lane_iota % half == 0
    for at in range(2 * slices):
        resp[at] = own_half[at] + main_recv[at]

    def spread(field, at):
        return pltpu.roll(field, n - at, 1) if at else field

    @pl.when(me >= middle)
    def _():
        row_copy(middle).wait_recv()
        other = jnp.where(me == middle, row_self[...], row_recv[...])
        for at in range(2 * slices):
            resp[at] = jnp.where(slot_zero, own_half[at] + spread(other, at), resp[at])

    @pl.when(me == middle)
    def _():
        for at in range(2 * slices):
            edge = spread(row_recv[...], at)
            here = resp[at]
            resp[at] = jnp.where(slot_zero, 0.5 * (here + edge), here)
            resp_mix[at] = jnp.where(slot_zero, 0.5 * (here - edge), 0.0)

    for i in (7, 8):
        fetch(i).wait()
    for m, group in enumerate(GROUPS):
        whole(m).wait_recv()
        for at, d in enumerate(group):
            re, im = x_forward(recvs[m][:, 2 * at, :], recvs[m][:, 2 * at + 1, :])
            spec[0, d] = re
            spec[1, d] = im

    @pl.when(me == middle)
    def _():
        re, im = x_forward_conj(
            [
                (recvs[m][:, 2 * at, :], recvs[m][:, 2 * at + 1, :])
                for m, group in enumerate(GROUPS)
                for at, _ in enumerate(group)
            ]
        )
        spec_mix[0] = re
        spec_mix[1] = im

    sum_re = sum_im = jnp.zeros((n, n), F32)
    for d in range(slices):
        re, im = spec[0, d], spec[1, d]
        rr, ri = resp[d], resp[slices + d]
        sum_re = sum_re + (re * rr - im * ri)
        sum_im = sum_im + (re * ri + im * rr)
    total[0] = sum_re
    total[1] = sum_im

    @pl.when(me == middle)
    def _():
        sum_re, sum_im = total[0], total[1]
        for d in range(slices):
            re, im = spread(spec_mix[0], d), spread(spec_mix[1], d)
            rr, ri = resp_mix[d], resp_mix[slices + d]
            sum_re = sum_re + (re * rr - im * ri)
            sum_im = sum_im + (re * ri + im * rr)
        total[0] = sum_re
        total[1] = sum_im

    x_inverse(total[0], total[1], parts, 0)
    start(parts)
    for i in (9, 10, 2, 3):
        fetch(i).wait()
    whole(parts).wait_recv()
    projection = y_inverse(parts, 0)
    quotient = []
    for a in range(q):
        cols = slice(a * n, (a + 1) * n)
        piece = projection[a * q : (a + 1) * q]
        proj_ref[:, cols] = piece
        quotient.append(meas_ref[:, cols] / jnp.maximum(piece + back_ref[:, cols], FLOOR))

    y_forward(jnp.concatenate(quotient, axis=0), parts + 1, 0)
    start(parts + 1)
    whole(parts + 1).wait_recv()
    re, im = x_forward(recvs[parts + 1][:, 0, :], recvs[parts + 1][:, 1, :])
    spec[0, 0] = re
    spec[1, 0] = im

    @pl.when(me == middle)
    def _():
        re, im = x_forward_conj([(recvs[parts + 1][:, 0, :], recvs[parts + 1][:, 1, :])])
        spec_mix[0] = re
        spec_mix[1] = im

    for m, group in enumerate(GROUPS, start=parts + 2):
        for at, d in enumerate(group):
            re, im = spec[0, 0], spec[1, 0]
            rr, ri = resp[d], resp[slices + d]
            total[0] = re * rr + im * ri
            total[1] = im * rr - re * ri

            @pl.when(me == middle)
            def _():
                re, im = spec_mix[0], spec_mix[1]
                rr, ri = resp_mix[d], resp_mix[slices + d]
                total[0] = total[0] + (re * rr + im * ri)
                total[1] = total[1] + (im * rr - re * ri)

            x_inverse(total[0], total[1], m, at)
        start(m)
    for m, group in enumerate(GROUPS, start=parts + 2):
        whole(m).wait_recv()
        for at, d in enumerate(group):
            correction = y_inverse(m, at)
            for a in range(q):
                cols = slice(a * n, (a + 1) * n)
                out_ref[d, :, cols] = vol_ref[d, :, cols] * correction[a * q : (a + 1) * q]
    for m in range(messages):
        whole(m).wait_send()
    main_copy(n - 1 - me).wait_send()

    @pl.when(me < middle)
    def _():
        row_copy(middle).wait_send()


def shards(volume, psf_spectra, background, measured):
    n = lax.axis_size("row")
    slices, q, length = volume.shape
    consts = tables(n, q)
    args = (volume, psf_spectra, background, measured, *consts)
    grouped = [2 * len(group) for group in GROUPS]
    counts = grouped + [2, 2] + grouped
    in_vmem = pl.BlockSpec(memory_space=pltpu.VMEM)
    in_hbm = pl.BlockSpec(memory_space=pltpu.HBM)
    exchanged = [pltpu.VMEM((n, count, n), F32) for count in counts]
    tile = lambda *lead: pltpu.VMEM((*lead, n, n), F32)
    return pl.pallas_call(
        functools.partial(kernel, n, q, slices, counts),
        out_shape=(
            jax.ShapeDtypeStruct(volume.shape, F32),
            jax.ShapeDtypeStruct(measured.shape, F32),
        ),
        in_specs=[in_hbm] * len(args),
        out_specs=(in_vmem, in_vmem),
        scratch_shapes=[pltpu.VMEM(arg.shape, arg.dtype) for arg in args]
        + exchanged
        + exchanged
        + [
            tile(2 * slices),
            tile(2 * slices),
            tile(2 * slices),
            tile(),
            tile(),
            tile(),
            tile(2 * slices),
            tile(2 * slices),
            tile(2, slices),
            tile(2),
            tile(2),
            pltpu.SemaphoreType.DMA((len(args),)),
            pltpu.SemaphoreType.DMA((len(counts),)),
            pltpu.SemaphoreType.DMA((len(counts),)),
            pltpu.SemaphoreType.DMA((2,)),
            pltpu.SemaphoreType.DMA((2,)),
            pltpu.SemaphoreType.REGULAR,
        ],
        compiler_params=pltpu.CompilerParams(
            collective_id=0, has_side_effects=True, vmem_limit_bytes=60 * 1024 * 1024
        ),
    )(*args)


def solution(mesh):
    in_specs = (
        P("vol", "row", None),
        P(None, None, "row", None),
        P("row", None),
        P(("vol", "row"), None),
    )
    out_specs = (P("vol", "row", None), P(("vol", "row"), None))
    return jax.shard_map(shards, mesh=mesh, in_specs=in_specs, out_specs=out_specs, check_vma=False)
```

```python
import functools

import jax
import jax.numpy as jnp
import ml_dtypes
import numpy as np
from jax import lax
from jax.experimental import pallas as pl
from jax.experimental.pallas import tpu as pltpu
from jax.sharding import PartitionSpec as P

FLOOR = 0.5
F32 = jnp.float32
BF16 = jnp.bfloat16
NN = (((1,), (0,)), ((), ()))
NT = (((1,), (1,)), ((), ()))
HEAD_GROUPS = ((0, 1, 2),)
TAIL_GROUPS = ((0, 1), (2,))


def split_np(table):
    hi = table.astype(np.float32).astype(ml_dtypes.bfloat16)
    lo = (table - hi.astype(np.float64)).astype(np.float32).astype(ml_dtypes.bfloat16)
    return np.stack([hi, lo])


def tables(n, q):
    length = n * q
    half = q // 2
    lanes = half * q
    big = np.exp(-2j * np.pi * np.outer(np.arange(n), np.arange(n)) / n)
    small = np.exp(-2j * np.pi * np.outer(np.arange(q), np.arange(q)) / q)
    big_stack = np.block([[big.real, -big.imag], [big.imag, big.real]])
    spread = np.kron(small[: half + 1], np.eye(q))
    ycols = np.concatenate([spread.real, spread.imag], axis=0)
    yrows = np.zeros((q * q, 2, 2 * lanes))
    yrows[:, 0, : (half + 1) * q] = spread.real.T
    yrows[:, 1, : (half + 1) * q] = spread.imag.T
    mixed = np.einsum("xk,ij->ixkj", small, np.eye(half)).reshape(lanes, q * half)
    xmix = np.block([[mixed.real, mixed.imag], [-mixed.imag, mixed.real]])
    twist = np.exp(-2j * np.pi * np.outer(np.arange(q), np.arange(n)) / length)
    ytw = np.repeat(twist[: half + 1], q, axis=0)
    ytwt = np.zeros((n, 2 * lanes), complex)
    ytwt[:, : (half + 1) * q] = ytw.T
    xtw = np.tile(twist.T, (1, half))
    pair = lambda z: np.stack([z.real, z.imag]).astype(np.float32)
    return (
        split_np(ycols),
        pair(ytw),
        split_np(big_stack),
        pair(xtw),
        split_np(xmix),
        pair(ytwt),
        split_np(yrows.reshape(q * q, 4 * lanes)),
    )


def split(value):
    hi = value.astype(BF16)
    return hi, (value - hi.astype(F32)).astype(BF16)


def dot(left, right, dims):
    return lax.dot_general(left, right, dimension_numbers=dims, preferred_element_type=F32)


def dot3(left, right, dims):
    return dot(left[0], right[0], dims) + dot(left[0], right[1], dims) + dot(left[1], right[0], dims)


def kernel(n, q, slices, counts, shares, *refs):
    ins, refs = refs[:11], refs[11:]
    out_ref, proj_ref = refs[:2]
    held, refs = refs[2:13], refs[13:]
    messages = len(counts)
    sends, recvs = refs[:messages], refs[messages : 2 * messages]
    (
        own_half, main_send, main_recv, row_send, row_self, row_recv, resp, resp_mix, spec, spec_mix, total,
        in_sems, send_sems, recv_sems, psf_sems, pass_sems, row_sems, late_sem, both_sem, pass_sem,
    ) = refs[2 * messages :]
    vol_ref, psf_ref, back_ref, meas_ref, ycol_ref, ytw_ref, big_ref, xtw_ref, xmix_ref, ytwt_ref, yrow_ref = held
    order = (1, 0, 4, 5, 6, 7, 8, 9, 10, 2, 3)
    parts = len(HEAD_GROUPS)
    half = q // 2
    middle = n // 2
    scale = 1.0 / (n * q * n * q)
    me = lax.axis_index("row")
    vol_id = lax.axis_index("vol")
    share = lax.rem(vol_id, shares)
    other_vol = vol_id + (1 - 2 * share)
    tiles = range(2 * slices)

    def owned(at, mine=True):
        owner = 0 if shares == 1 or at < 2 * slices * 2 // 3 else 1
        return (share == owner) if mine else (share != owner)

    row_iota = lax.broadcasted_iota(jnp.int32, (n, n), 0)
    lane_iota = lax.broadcasted_iota(jnp.int32, (n, n), 1)

    def fetch(i):
        return pltpu.make_async_copy(ins[i], held[i], in_sems.at[i])

    for i in order:
        fetch(i).start()

    def device(dst, vol=None):
        return (vol_id if vol is None else vol, dst)

    def tell(sem, dst, vol=None):
        pl.semaphore_signal(sem, inc=1, device_id=device(dst, vol), device_id_type=pl.DeviceIdType.MESH)

    barrier = pltpu.get_barrier_semaphore()

    def peer(step):
        return jnp.bitwise_and(me + step, n - 1)

    @pl.when(me < 2)
    def _():
        tell(barrier, 1 - me)

    if shares == 2:

        @pl.when(me == 2)
        def _():
            tell(barrier, me, other_vol)

    @pl.when(me >= 2)
    def _():
        @pl.loop(1, n)
        def _(step):
            tell(barrier, peer(step))

    def copy_to(m, dst):
        return pltpu.make_async_remote_copy(
            src_ref=sends[m].at[dst],
            dst_ref=recvs[m].at[me],
            send_sem=send_sems.at[m],
            recv_sem=recv_sems.at[m],
            device_id=device(dst),
            device_id_type=pl.DeviceIdType.MESH,
        )

    def start(m):
        @pl.loop(1, n, unroll=8)
        def _(step):
            copy_to(m, peer(step)).start()

        recvs[m][me] = sends[m][me]

    def whole(m):
        return pltpu.make_async_remote_copy(
            src_ref=sends[m].at[pl.ds(0, n - 1)],
            dst_ref=recvs[m].at[pl.ds(0, n - 1)],
            send_sem=send_sems.at[m],
            recv_sem=recv_sems.at[m],
            device_id=device(peer(1)),
            device_id_type=pl.DeviceIdType.MESH,
        )

    def main_copy(at):
        return pltpu.make_async_remote_copy(
            src_ref=main_send.at[at],
            dst_ref=main_recv.at[at],
            send_sem=psf_sems.at[0, at],
            recv_sem=psf_sems.at[1, at],
            device_id=device(n - 1 - me),
            device_id_type=pl.DeviceIdType.MESH,
        )

    def pass_copy(at):
        return pltpu.make_async_remote_copy(
            src_ref=main_recv.at[at],
            dst_ref=main_recv.at[at],
            send_sem=pass_sems.at[0, at],
            recv_sem=pass_sems.at[1, at],
            device_id=device(me, other_vol),
            device_id_type=pl.DeviceIdType.MESH,
        )

    def each_tile(act, mine=True):
        for at in tiles:
            pl.when(owned(at, mine))(functools.partial(act, at))

    def row_copy(dst):
        return pltpu.make_async_remote_copy(
            src_ref=row_send,
            dst_ref=row_recv,
            send_sem=row_sems.at[0],
            recv_sem=row_sems.at[1],
            device_id=device(dst),
            device_id_type=pl.DeviceIdType.MESH,
        )

    def table(ref):
        return ref[0], ref[1]

    def y_forward(field, m, at):
        mixed = dot3(table(ycol_ref), split(field), NN)
        kept = (half + 1) * q
        re, im = mixed[:kept], mixed[kept:]
        wr, wi = ytw_ref[0], ytw_ref[1]
        turned = jnp.concatenate([re * wr - im * wi, re * wi + im * wr], axis=1)
        both = jnp.concatenate([turned[: half * q], turned[half * q :], turned[q : half * q]], axis=0)
        got = dot3(table(big_ref), split(both), NT)
        lanes = half * q
        re = jnp.concatenate([got[:middle, lanes:], got[middle:n, :lanes]], axis=0)
        im = jnp.concatenate([got[n : n + middle, lanes:], got[n + middle :, :lanes]], axis=0)
        im = jnp.where((row_iota == middle) & (lane_iota < q), got[0:1, :lanes], im)
        sends[m][:, 2 * at, :] = re
        sends[m][:, 2 * at + 1, :] = im

    def x_forward(re, im):
        got = dot3(table(big_ref), split(jnp.concatenate([re, im], axis=0)), NN)
        re, im = got[:n], got[n:]
        wr, wi = xtw_ref[0], xtw_ref[1]
        turned = jnp.concatenate([re * wr - im * wi, re * wi + im * wr], axis=1)
        out = dot3(split(turned), table(xmix_ref), NN)
        return out[:, :n], out[:, n:]

    def x_forward_conj(fields):
        re_sum = im_sum = jnp.zeros((n, n), F32)
        for d, (re, im) in enumerate(fields):
            mine = (lane_iota >= d * q) & (lane_iota < (d + 1) * q)
            if d:
                re, im = pltpu.roll(re, d * q, 1), pltpu.roll(im, d * q, 1)
            re_sum = jnp.where(mine, re, re_sum)
            im_sum = jnp.where(mine, -im, im_sum)
        return x_forward(re_sum, im_sum)

    def x_inverse(re, im, m, at):
        mixed = dot3(split(jnp.concatenate([re, im], axis=1)), table(xmix_ref), NT)
        wr, wi = xtw_ref[0], xtw_ref[1]
        re, im = mixed[:, :n], mixed[:, n:]
        swapped = jnp.concatenate([im * wr - re * wi, re * wr + im * wi], axis=0)
        got = dot3(table(big_ref), split(swapped), NN)
        sends[m][:, 2 * at, :] = got[n:]
        sends[m][:, 2 * at + 1, :] = got[:n]

    def y_inverse(m, at):
        re, im = recvs[m][:, 2 * at, :], recvs[m][:, 2 * at + 1, :]
        first = lane_iota < q
        upper = first & (row_iota < middle)
        zero_row = first & (row_iota == 0)
        mid_row = first & (row_iota == middle)
        re_low = jnp.where(upper, 0.0, re)
        re_low = jnp.where(mid_row, 0.5 * re, re_low)
        re_low = jnp.where(zero_row, 0.5 * im[middle : middle + 1], re_low)
        im_low = jnp.where(upper | mid_row, 0.0, im)
        re_high, im_high = jnp.where(upper, re, 0.0), jnp.where(upper, im, 0.0)
        swapped = jnp.concatenate(
            [
                jnp.concatenate([im_low, im_high], axis=1),
                jnp.concatenate([re_low, re_high], axis=1),
            ],
            axis=0,
        )
        got = dot3(table(big_ref), split(swapped), NN)
        im, re = got[:n], got[n:]
        wr, wi = ytwt_ref[0], ytwt_ref[1]
        turned = jnp.concatenate([re * wr + im * wi, im * wr - re * wi], axis=1)
        return dot3(table(yrow_ref), split(turned), NT) * (2.0 * scale)

    fetch(1).wait()
    reverse = jnp.where((row_iota + lane_iota == n) | (row_iota + lane_iota == 0), 1.0, 0.0).astype(BF16)
    same_block = row_iota // half == lane_iota // half
    slot_sum = row_iota % half + lane_iota % half
    slot_flip = jnp.where(same_block & ((slot_sum == half) | (slot_sum == 0)), 1.0, 0.0).astype(BF16)

    def blocks(field, backwards):
        places = range(q - 1, -1, -1) if backwards else range(q)
        return jnp.concatenate([field[:, k * n : (k + 1) * n] for k in places], axis=0)

    def mend(field):
        return jnp.where(row_iota == 0, pltpu.roll(field, half, 1), field)

    sub_iota = lax.broadcasted_iota(jnp.int32, (half, n * q), 0)
    rows = []
    for part in range(2):
        for d in range(slices):
            at = part * slices + d
            both = psf_ref[part, d].astype(F32)
            low, high = both[:half], both[half:]
            rows.append(low[0:1])
            own = jnp.where((sub_iota == 0) & (me < middle), high, low)
            own_half[at] = 0.5 * blocks(own, False).T

    def prepare(at):
        high = psf_ref[at // slices, at % slices].astype(F32)[half:]
        turned = dot(reverse, blocks(high, True).astype(BF16), NT)
        turned = dot(turned.astype(BF16), slot_flip, NN)
        main_send[at] = (0.5 if at < slices else -0.5) * mend(turned)

    each_tile(prepare)
    packed = jnp.concatenate(rows + [jnp.zeros((half - 2 * slices, n * q), F32)], axis=0)
    turned = mend(dot(reverse, blocks(packed, True).astype(BF16), NT))
    mine = jnp.where(lane_iota % half < slices, 0.5, -0.5) * turned
    row_self[...] = mine
    row_send[...] = jnp.where(me == 0, mine + 0.5 * blocks(packed, False).T, mine)

    @pl.when(me == 2)
    def _():
        pl.semaphore_wait(barrier, n - 4 + shares)

    @pl.when(me > 2)
    def _():
        pl.semaphore_wait(barrier, n - 3)

    @pl.when(me < 2)
    def _():
        pl.semaphore_wait(barrier, n - 1)

    @pl.when(me == 1)
    def _():
        @pl.loop(2, n)
        def _(dst):
            tell(late_sem, dst)

    @pl.when(me >= n - 2)
    def _():
        pl.semaphore_wait(late_sem, 1)

    each_tile(lambda at: main_copy(at).start())

    @pl.when(me == 0)
    def _():
        row_copy(middle).start()

    @pl.when((me > 0) & (me < middle))
    def _():
        row_copy(n - me).start()

    for i in (0, 4, 5, 6):
        fetch(i).wait()
    for m, group in enumerate(HEAD_GROUPS):
        for at, d in enumerate(group):
            y_forward(
                jnp.concatenate([vol_ref[d, :, a * n : (a + 1) * n] for a in range(q)], axis=0), m, at
            )

    for m in range(parts):

        @pl.when(me >= 2)
        def _():
            @pl.loop(1, n - 2, unroll=5)
            def _(step):
                place = me + step
                copy_to(m, jnp.where(place >= n, place - (n - 2), place)).start()

        @pl.when(me < 2)
        def _():
            @pl.loop(1, n, unroll=8)
            def _(step):
                copy_to(m, peer(step)).start()

        recvs[m][me] = sends[m][me]

    @pl.when((me >= 2) & (me < n - 2))
    def _():
        pl.semaphore_wait(late_sem, 1)

    if shares == 2:

        @pl.when(me == 2)
        def _():
            tell(both_sem, me, other_vol)
            pl.semaphore_wait(both_sem, 1)

            @pl.loop(1, n)
            def _(step):
                tell(pass_sem, peer(step))

    @pl.when(me >= 2)
    def _():
        for dst in range(2):
            for m in range(parts):
                copy_to(m, dst).start()

    if shares == 2:

        @pl.when(me != 2)
        def _():
            pl.semaphore_wait(pass_sem, 1)

    def hand_on(at):
        main_copy(at).wait_recv()
        if shares == 2:
            pass_copy(at).start()

    each_tile(hand_on)
    for i in (7, 8):
        fetch(i).wait()

    def forward_group(m, group):
        whole(m).wait_recv()
        for at, d in enumerate(group):
            re, im = x_forward(recvs[m][:, 2 * at, :], recvs[m][:, 2 * at + 1, :])
            spec[0, d] = re
            spec[1, d] = im

    forward_group(0, HEAD_GROUPS[0])
    if shares == 2:
        each_tile(lambda at: pass_copy(at).wait_recv(), mine=False)
    slot_zero = lane_iota % half == 0
    for at in range(2 * slices):
        resp[at] = own_half[at] + main_recv[at]

    def spread(field, at):
        return pltpu.roll(field, n - at, 1) if at else field

    @pl.when(me >= middle)
    def _():
        row_copy(middle).wait_recv()
        other = jnp.where(me == middle, row_self[...], row_recv[...])
        for at in range(2 * slices):
            resp[at] = jnp.where(slot_zero, own_half[at] + spread(other, at), resp[at])

    @pl.when(me == middle)
    def _():
        for at in range(2 * slices):
            edge = spread(row_recv[...], at)
            here = resp[at]
            resp[at] = jnp.where(slot_zero, 0.5 * (here + edge), here)
            resp_mix[at] = jnp.where(slot_zero, 0.5 * (here - edge), 0.0)

    for m, group in enumerate(HEAD_GROUPS[1:], start=1):
        forward_group(m, group)

    @pl.when(me == middle)
    def _():
        re, im = x_forward_conj(
            [
                (recvs[m][:, 2 * at, :], recvs[m][:, 2 * at + 1, :])
                for m, group in enumerate(HEAD_GROUPS)
                for at, _ in enumerate(group)
            ]
        )
        spec_mix[0] = re
        spec_mix[1] = im

    sum_re = sum_im = jnp.zeros((n, n), F32)
    for d in range(slices):
        re, im = spec[0, d], spec[1, d]
        rr, ri = resp[d], resp[slices + d]
        sum_re = sum_re + (re * rr - im * ri)
        sum_im = sum_im + (re * ri + im * rr)
    total[0] = sum_re
    total[1] = sum_im

    @pl.when(me == middle)
    def _():
        sum_re, sum_im = total[0], total[1]
        for d in range(slices):
            re, im = spread(spec_mix[0], d), spread(spec_mix[1], d)
            rr, ri = resp_mix[d], resp_mix[slices + d]
            sum_re = sum_re + (re * rr - im * ri)
            sum_im = sum_im + (re * ri + im * rr)
        total[0] = sum_re
        total[1] = sum_im

    x_inverse(total[0], total[1], parts, 0)
    start(parts)
    for i in (9, 10, 2, 3):
        fetch(i).wait()
    whole(parts).wait_recv()
    projection = y_inverse(parts, 0)
    quotient = []
    for a in range(q):
        cols = slice(a * n, (a + 1) * n)
        piece = projection[a * q : (a + 1) * q]
        proj_ref[:, cols] = piece
        quotient.append(meas_ref[:, cols] / jnp.maximum(piece + back_ref[:, cols], FLOOR))

    y_forward(jnp.concatenate(quotient, axis=0), parts + 1, 0)
    start(parts + 1)
    whole(parts + 1).wait_recv()
    re, im = x_forward(recvs[parts + 1][:, 0, :], recvs[parts + 1][:, 1, :])
    spec[0, 0] = re
    spec[1, 0] = im

    @pl.when(me == middle)
    def _():
        re, im = x_forward_conj([(recvs[parts + 1][:, 0, :], recvs[parts + 1][:, 1, :])])
        spec_mix[0] = re
        spec_mix[1] = im

    for m, group in enumerate(TAIL_GROUPS, start=parts + 2):
        for at, d in enumerate(group):
            re, im = spec[0, 0], spec[1, 0]
            rr, ri = resp[d], resp[slices + d]
            total[0] = re * rr + im * ri
            total[1] = im * rr - re * ri

            @pl.when(me == middle)
            def _():
                re, im = spec_mix[0], spec_mix[1]
                rr, ri = resp_mix[d], resp_mix[slices + d]
                total[0] = total[0] + (re * rr + im * ri)
                total[1] = total[1] + (im * rr - re * ri)

            x_inverse(total[0], total[1], m, at)
        start(m)
    for m, group in enumerate(TAIL_GROUPS, start=parts + 2):
        whole(m).wait_recv()
        for at, d in enumerate(group):
            correction = y_inverse(m, at)
            for a in range(q):
                cols = slice(a * n, (a + 1) * n)
                out_ref[d, :, cols] = vol_ref[d, :, cols] * correction[a * q : (a + 1) * q]
    for m in range(messages):
        whole(m).wait_send()
    each_tile(lambda at: main_copy(at).wait_send())
    if shares == 2:
        each_tile(lambda at: pass_copy(at).wait_send())

    @pl.when(me < middle)
    def _():
        row_copy(middle).wait_send()


def shards(volume, psf_spectra, background, measured):
    n = lax.axis_size("row")
    slices, q, length = volume.shape
    shares = 2 if lax.axis_size("vol") % 2 == 0 else 1
    consts = tables(n, q)
    args = (volume, psf_spectra, background, measured, *consts)
    sizes = lambda groups: [2 * len(group) for group in groups]
    counts = sizes(HEAD_GROUPS) + [2, 2] + sizes(TAIL_GROUPS)
    in_vmem = pl.BlockSpec(memory_space=pltpu.VMEM)
    in_hbm = pl.BlockSpec(memory_space=pltpu.HBM)
    exchanged = [pltpu.VMEM((n, count, n), F32) for count in counts]
    tile = lambda *lead: pltpu.VMEM((*lead, n, n), F32)
    return pl.pallas_call(
        functools.partial(kernel, n, q, slices, counts, shares),
        out_shape=(
            jax.ShapeDtypeStruct(volume.shape, F32),
            jax.ShapeDtypeStruct(measured.shape, F32),
        ),
        in_specs=[in_hbm] * len(args),
        out_specs=(in_vmem, in_vmem),
        scratch_shapes=[pltpu.VMEM(arg.shape, arg.dtype) for arg in args]
        + exchanged
        + exchanged
        + [
            tile(2 * slices),
            tile(2 * slices),
            tile(2 * slices),
            tile(),
            tile(),
            tile(),
            tile(2 * slices),
            tile(2 * slices),
            tile(2, slices),
            tile(2),
            tile(2),
            pltpu.SemaphoreType.DMA((len(args),)),
            pltpu.SemaphoreType.DMA((len(counts),)),
            pltpu.SemaphoreType.DMA((len(counts),)),
            pltpu.SemaphoreType.DMA((2, 2 * slices)),
            pltpu.SemaphoreType.DMA((2, 2 * slices)),
            pltpu.SemaphoreType.DMA((2,)),
            pltpu.SemaphoreType.REGULAR,
            pltpu.SemaphoreType.REGULAR,
            pltpu.SemaphoreType.REGULAR,
        ],
        compiler_params=pltpu.CompilerParams(
            collective_id=0, has_side_effects=True, vmem_limit_bytes=60 * 1024 * 1024
        ),
    )(*args)


def solution(mesh):
    in_specs = (
        P("vol", "row", None),
        P(None, None, "row", None),
        P("row", None),
        P(("vol", "row"), None),
    )
    out_specs = (P("vol", "row", None), P(("vol", "row"), None))
    return jax.shard_map(shards, mesh=mesh, in_specs=in_specs, out_specs=out_specs, check_vma=False)
```

```python
import functools

import jax
import jax.numpy as jnp
import ml_dtypes
import numpy as np
from jax import lax
from jax.experimental import pallas as pl
from jax.experimental.pallas import tpu as pltpu
from jax.sharding import PartitionSpec as P

FLOOR = 0.5
F32 = jnp.float32
BF16 = jnp.bfloat16
NN = (((1,), (0,)), ((), ()))
NT = (((1,), (1,)), ((), ()))
HEAD_GROUPS = ((0, 1, 2),)
TAIL_GROUPS = ((0,), (1, 2))


def split_np(table):
    hi = table.astype(np.float32).astype(ml_dtypes.bfloat16)
    lo = (table - hi.astype(np.float64)).astype(np.float32).astype(ml_dtypes.bfloat16)
    return np.stack([hi, lo])


def tables(n, q):
    length = n * q
    half = q // 2
    lanes = half * q
    big = np.exp(-2j * np.pi * np.outer(np.arange(n), np.arange(n)) / n)
    small = np.exp(-2j * np.pi * np.outer(np.arange(q), np.arange(q)) / q)
    big_stack = np.block([[big.real, -big.imag], [big.imag, big.real]])
    spread = np.kron(small[: half + 1], np.eye(q))
    ycols = np.concatenate([spread.real, spread.imag], axis=0)
    yrows = np.zeros((q * q, 2, 2 * lanes))
    yrows[:, 0, : (half + 1) * q] = spread.real.T
    yrows[:, 1, : (half + 1) * q] = spread.imag.T
    mixed = np.einsum("xk,ij->ixkj", small, np.eye(half)).reshape(lanes, q * half)
    xmix = np.block([[mixed.real, mixed.imag], [-mixed.imag, mixed.real]])
    twist = np.exp(-2j * np.pi * np.outer(np.arange(q), np.arange(n)) / length)
    ytw = np.repeat(twist[: half + 1], q, axis=0)
    ytwt = np.zeros((n, 2 * lanes), complex)
    ytwt[:, : (half + 1) * q] = ytw.T
    xtw = np.tile(twist.T, (1, half))
    pair = lambda z: np.stack([z.real, z.imag]).astype(np.float32)
    return (
        split_np(ycols),
        pair(ytw),
        split_np(big_stack),
        pair(xtw),
        split_np(xmix),
        pair(ytwt),
        split_np(yrows.reshape(q * q, 4 * lanes)),
    )


def split(value):
    hi = value.astype(BF16)
    return hi, (value - hi.astype(F32)).astype(BF16)


def dot(left, right, dims):
    return lax.dot_general(left, right, dimension_numbers=dims, preferred_element_type=F32)


def dot3(left, right, dims):
    return dot(left[0], right[0], dims) + dot(left[0], right[1], dims) + dot(left[1], right[0], dims)


def kernel(n, q, slices, counts, shares, *refs):
    ins, refs = refs[:11], refs[11:]
    out_ref, proj_ref = refs[:2]
    held, refs = refs[2:13], refs[13:]
    messages = len(counts)
    sends, recvs = refs[:messages], refs[messages : 2 * messages]
    (
        own_half, main_send, main_recv, row_send, row_self, row_recv, resp, resp_mix, spec, spec_mix, total,
        in_sems, send_sems, recv_sems, psf_sems, pass_sems, row_sems, late_sem, both_sem, pass_sem,
    ) = refs[2 * messages :]
    vol_ref, psf_ref, back_ref, meas_ref, ycol_ref, ytw_ref, big_ref, xtw_ref, xmix_ref, ytwt_ref, yrow_ref = held
    order = (1, 0, 4, 5, 6, 7, 8, 9, 10, 2, 3)
    parts = len(HEAD_GROUPS)
    half = q // 2
    middle = n // 2
    scale = 1.0 / (n * q * n * q)
    me = lax.axis_index("row")
    vol_id = lax.axis_index("vol")
    share = lax.rem(vol_id, shares)
    other_vol = vol_id + (1 - 2 * share)
    tiles = range(2 * slices)

    def owned(at, mine=True):
        owner = 0 if shares == 1 or at < 2 * slices * 2 // 3 else 1
        return (share == owner) if mine else (share != owner)

    row_iota = lax.broadcasted_iota(jnp.int32, (n, n), 0)
    lane_iota = lax.broadcasted_iota(jnp.int32, (n, n), 1)

    def fetch(i):
        return pltpu.make_async_copy(ins[i], held[i], in_sems.at[i])

    for i in order:
        fetch(i).start()

    def device(dst, vol=None):
        return (vol_id if vol is None else vol, dst)

    def tell(sem, dst, vol=None):
        pl.semaphore_signal(sem, inc=1, device_id=device(dst, vol), device_id_type=pl.DeviceIdType.MESH)

    barrier = pltpu.get_barrier_semaphore()

    def peer(step):
        return jnp.bitwise_and(me + step, n - 1)

    @pl.when(me < 2)
    def _():
        tell(barrier, 1 - me)

    if shares == 2:

        @pl.when(me == 2)
        def _():
            tell(barrier, me, other_vol)

    @pl.when(me >= 2)
    def _():
        @pl.loop(1, n, unroll=8)
        def _(step):
            tell(barrier, peer(step))

    def copy_to(m, dst):
        return pltpu.make_async_remote_copy(
            src_ref=sends[m].at[dst],
            dst_ref=recvs[m].at[me],
            send_sem=send_sems.at[m],
            recv_sem=recv_sems.at[m],
            device_id=device(dst),
            device_id_type=pl.DeviceIdType.MESH,
        )

    def start(m):
        @pl.loop(1, n, unroll=8)
        def _(step):
            copy_to(m, peer(step)).start()

        recvs[m][me] = sends[m][me]

    def whole(m):
        return pltpu.make_async_remote_copy(
            src_ref=sends[m].at[pl.ds(0, n - 1)],
            dst_ref=recvs[m].at[pl.ds(0, n - 1)],
            send_sem=send_sems.at[m],
            recv_sem=recv_sems.at[m],
            device_id=device(peer(1)),
            device_id_type=pl.DeviceIdType.MESH,
        )

    def main_copy(at):
        return pltpu.make_async_remote_copy(
            src_ref=main_send.at[at],
            dst_ref=main_recv.at[at],
            send_sem=psf_sems.at[0, at],
            recv_sem=psf_sems.at[1, at],
            device_id=device(n - 1 - me),
            device_id_type=pl.DeviceIdType.MESH,
        )

    def pass_copy(at):
        return pltpu.make_async_remote_copy(
            src_ref=main_recv.at[at],
            dst_ref=main_recv.at[at],
            send_sem=pass_sems.at[0, at],
            recv_sem=pass_sems.at[1, at],
            device_id=device(me, other_vol),
            device_id_type=pl.DeviceIdType.MESH,
        )

    def each_tile(act, mine=True):
        for at in tiles:
            pl.when(owned(at, mine))(functools.partial(act, at))

    def row_copy(dst):
        return pltpu.make_async_remote_copy(
            src_ref=row_send,
            dst_ref=row_recv,
            send_sem=row_sems.at[0],
            recv_sem=row_sems.at[1],
            device_id=device(dst),
            device_id_type=pl.DeviceIdType.MESH,
        )

    def table(ref):
        return ref[0], ref[1]

    def y_forward(field, m, at):
        mixed = dot3(table(ycol_ref), split(field), NN)
        kept = (half + 1) * q
        re, im = mixed[:kept], mixed[kept:]
        wr, wi = ytw_ref[0], ytw_ref[1]
        turned = jnp.concatenate([re * wr - im * wi, re * wi + im * wr], axis=1)
        both = jnp.concatenate([turned[: half * q], turned[half * q :], turned[q : half * q]], axis=0)
        got = dot3(table(big_ref), split(both), NT)
        lanes = half * q
        re = jnp.concatenate([got[:middle, lanes:], got[middle:n, :lanes]], axis=0)
        im = jnp.concatenate([got[n : n + middle, lanes:], got[n + middle :, :lanes]], axis=0)
        im = jnp.where((row_iota == middle) & (lane_iota < q), got[0:1, :lanes], im)
        sends[m][:, 2 * at, :] = re
        sends[m][:, 2 * at + 1, :] = im

    def x_forward(re, im):
        got = dot3(table(big_ref), split(jnp.concatenate([re, im], axis=0)), NN)
        re, im = got[:n], got[n:]
        wr, wi = xtw_ref[0], xtw_ref[1]
        turned = jnp.concatenate([re * wr - im * wi, re * wi + im * wr], axis=1)
        out = dot3(split(turned), table(xmix_ref), NN)
        return out[:, :n], out[:, n:]

    def x_forward_conj(fields):
        re_sum = im_sum = jnp.zeros((n, n), F32)
        for d, (re, im) in enumerate(fields):
            mine = (lane_iota >= d * q) & (lane_iota < (d + 1) * q)
            if d:
                re, im = pltpu.roll(re, d * q, 1), pltpu.roll(im, d * q, 1)
            re_sum = jnp.where(mine, re, re_sum)
            im_sum = jnp.where(mine, -im, im_sum)
        return x_forward(re_sum, im_sum)

    def x_inverse(re, im, m, at):
        mixed = dot3(split(jnp.concatenate([re, im], axis=1)), table(xmix_ref), NT)
        wr, wi = xtw_ref[0], xtw_ref[1]
        re, im = mixed[:, :n], mixed[:, n:]
        swapped = jnp.concatenate([im * wr - re * wi, re * wr + im * wi], axis=0)
        got = dot3(table(big_ref), split(swapped), NN)
        sends[m][:, 2 * at, :] = got[n:]
        sends[m][:, 2 * at + 1, :] = got[:n]

    def y_inverse(m, at):
        re, im = recvs[m][:, 2 * at, :], recvs[m][:, 2 * at + 1, :]
        first = lane_iota < q
        upper = first & (row_iota < middle)
        zero_row = first & (row_iota == 0)
        mid_row = first & (row_iota == middle)
        re_low = jnp.where(upper, 0.0, re)
        re_low = jnp.where(mid_row, 0.5 * re, re_low)
        re_low = jnp.where(zero_row, 0.5 * im[middle : middle + 1], re_low)
        im_low = jnp.where(upper | mid_row, 0.0, im)
        re_high, im_high = jnp.where(upper, re, 0.0), jnp.where(upper, im, 0.0)
        swapped = jnp.concatenate(
            [
                jnp.concatenate([im_low, im_high], axis=1),
                jnp.concatenate([re_low, re_high], axis=1),
            ],
            axis=0,
        )
        got = dot3(table(big_ref), split(swapped), NN)
        im, re = got[:n], got[n:]
        wr, wi = ytwt_ref[0], ytwt_ref[1]
        turned = jnp.concatenate([re * wr + im * wi, im * wr - re * wi], axis=1)
        return dot3(table(yrow_ref), split(turned), NT) * (2.0 * scale)

    fetch(1).wait()
    reverse = jnp.where((row_iota + lane_iota == n) | (row_iota + lane_iota == 0), 1.0, 0.0).astype(BF16)
    same_block = row_iota // half == lane_iota // half
    slot_sum = row_iota % half + lane_iota % half
    slot_flip = jnp.where(same_block & ((slot_sum == half) | (slot_sum == 0)), 1.0, 0.0).astype(BF16)

    def blocks(field, backwards):
        places = range(q - 1, -1, -1) if backwards else range(q)
        return jnp.concatenate([field[:, k * n : (k + 1) * n] for k in places], axis=0)

    def mend(field):
        return jnp.where(row_iota == 0, pltpu.roll(field, half, 1), field)

    sub_iota = lax.broadcasted_iota(jnp.int32, (half, n * q), 0)
    rows = []
    for part in range(2):
        for d in range(slices):
            at = part * slices + d
            both = psf_ref[part, d].astype(F32)
            low, high = both[:half], both[half:]
            rows.append(low[0:1])
            own = jnp.where((sub_iota == 0) & (me < middle), high, low)
            own_half[at] = 0.5 * blocks(own, False).T

    def prepare(at):
        high = psf_ref[at // slices, at % slices].astype(F32)[half:]
        turned = dot(reverse, blocks(high, True).astype(BF16), NT)
        turned = dot(turned.astype(BF16), slot_flip, NN)
        main_send[at] = (0.5 if at < slices else -0.5) * mend(turned)

    each_tile(prepare)
    packed = jnp.concatenate(rows + [jnp.zeros((half - 2 * slices, n * q), F32)], axis=0)
    turned = mend(dot(reverse, blocks(packed, True).astype(BF16), NT))
    mine = jnp.where(lane_iota % half < slices, 0.5, -0.5) * turned
    row_self[...] = mine
    row_send[...] = jnp.where(me == 0, mine + 0.5 * blocks(packed, False).T, mine)

    @pl.when(me == 2)
    def _():
        pl.semaphore_wait(barrier, n - 4 + shares)

    @pl.when(me > 2)
    def _():
        pl.semaphore_wait(barrier, n - 3)

    @pl.when(me < 2)
    def _():
        pl.semaphore_wait(barrier, n - 1)

    @pl.when(me == 1)
    def _():
        @pl.loop(2, n, unroll=6)
        def _(dst):
            tell(late_sem, dst)

    @pl.when(me >= n - 2)
    def _():
        pl.semaphore_wait(late_sem, 1)

    each_tile(lambda at: main_copy(at).start())

    @pl.when(me == 0)
    def _():
        row_copy(middle).start()

    @pl.when((me > 0) & (me < middle))
    def _():
        row_copy(n - me).start()

    for i in (0, 4, 5, 6):
        fetch(i).wait()
    for m, group in enumerate(HEAD_GROUPS):
        for at, d in enumerate(group):
            y_forward(
                jnp.concatenate([vol_ref[d, :, a * n : (a + 1) * n] for a in range(q)], axis=0), m, at
            )

    for m in range(parts):

        @pl.when(me >= 2)
        def _():
            @pl.loop(1, n - 2, unroll=5)
            def _(step):
                place = me + step
                copy_to(m, jnp.where(place >= n, place - (n - 2), place)).start()

        @pl.when(me < 2)
        def _():
            @pl.loop(1, n, unroll=8)
            def _(step):
                copy_to(m, peer(step)).start()

        recvs[m][me] = sends[m][me]

    @pl.when((me >= 2) & (me < n - 2))
    def _():
        pl.semaphore_wait(late_sem, 1)

    if shares == 2:

        @pl.when(me == 2)
        def _():
            tell(both_sem, me, other_vol)
            pl.semaphore_wait(both_sem, 1)

            @pl.loop(1, n, unroll=8)
            def _(step):
                tell(pass_sem, peer(step))

    @pl.when(me >= 2)
    def _():
        for dst in range(2):
            for m in range(parts):
                copy_to(m, dst).start()

    if shares == 2:

        @pl.when(me != 2)
        def _():
            pl.semaphore_wait(pass_sem, 1)

    def hand_on(at):
        main_copy(at).wait_recv()
        if shares == 2:
            pass_copy(at).start()

    each_tile(hand_on)
    for i in (7, 8):
        fetch(i).wait()

    def forward_group(m, group):
        whole(m).wait_recv()
        for at, d in enumerate(group):
            re, im = x_forward(recvs[m][:, 2 * at, :], recvs[m][:, 2 * at + 1, :])
            spec[0, d] = re
            spec[1, d] = im

    forward_group(0, HEAD_GROUPS[0])
    if shares == 2:
        each_tile(lambda at: pass_copy(at).wait_recv(), mine=False)
    slot_zero = lane_iota % half == 0
    for at in range(2 * slices):
        resp[at] = own_half[at] + main_recv[at]

    def spread(field, at):
        return pltpu.roll(field, n - at, 1) if at else field

    @pl.when(me >= middle)
    def _():
        row_copy(middle).wait_recv()
        other = jnp.where(me == middle, row_self[...], row_recv[...])
        for at in range(2 * slices):
            resp[at] = jnp.where(slot_zero, own_half[at] + spread(other, at), resp[at])

    @pl.when(me == middle)
    def _():
        for at in range(2 * slices):
            edge = spread(row_recv[...], at)
            here = resp[at]
            resp[at] = jnp.where(slot_zero, 0.5 * (here + edge), here)
            resp_mix[at] = jnp.where(slot_zero, 0.5 * (here - edge), 0.0)

    for m, group in enumerate(HEAD_GROUPS[1:], start=1):
        forward_group(m, group)

    @pl.when(me == middle)
    def _():
        re, im = x_forward_conj(
            [
                (recvs[m][:, 2 * at, :], recvs[m][:, 2 * at + 1, :])
                for m, group in enumerate(HEAD_GROUPS)
                for at, _ in enumerate(group)
            ]
        )
        spec_mix[0] = re
        spec_mix[1] = im

    sum_re = sum_im = jnp.zeros((n, n), F32)
    for d in range(slices):
        re, im = spec[0, d], spec[1, d]
        rr, ri = resp[d], resp[slices + d]
        sum_re = sum_re + (re * rr - im * ri)
        sum_im = sum_im + (re * ri + im * rr)
    total[0] = sum_re
    total[1] = sum_im

    @pl.when(me == middle)
    def _():
        sum_re, sum_im = total[0], total[1]
        for d in range(slices):
            re, im = spread(spec_mix[0], d), spread(spec_mix[1], d)
            rr, ri = resp_mix[d], resp_mix[slices + d]
            sum_re = sum_re + (re * rr - im * ri)
            sum_im = sum_im + (re * ri + im * rr)
        total[0] = sum_re
        total[1] = sum_im

    x_inverse(total[0], total[1], parts, 0)
    start(parts)
    for i in (9, 10, 2, 3):
        fetch(i).wait()
    whole(parts).wait_recv()
    projection = y_inverse(parts, 0)
    quotient = []
    for a in range(q):
        cols = slice(a * n, (a + 1) * n)
        piece = projection[a * q : (a + 1) * q]
        proj_ref[:, cols] = piece
        quotient.append(meas_ref[:, cols] / jnp.maximum(piece + back_ref[:, cols], FLOOR))

    y_forward(jnp.concatenate(quotient, axis=0), parts + 1, 0)
    start(parts + 1)
    whole(parts + 1).wait_recv()
    re, im = x_forward(recvs[parts + 1][:, 0, :], recvs[parts + 1][:, 1, :])
    spec[0, 0] = re
    spec[1, 0] = im

    @pl.when(me == middle)
    def _():
        re, im = x_forward_conj([(recvs[parts + 1][:, 0, :], recvs[parts + 1][:, 1, :])])
        spec_mix[0] = re
        spec_mix[1] = im

    for m, group in enumerate(TAIL_GROUPS, start=parts + 2):
        for at, d in enumerate(group):
            re, im = spec[0, 0], spec[1, 0]
            rr, ri = resp[d], resp[slices + d]
            total[0] = re * rr + im * ri
            total[1] = im * rr - re * ri

            @pl.when(me == middle)
            def _():
                re, im = spec_mix[0], spec_mix[1]
                rr, ri = resp_mix[d], resp_mix[slices + d]
                total[0] = total[0] + (re * rr + im * ri)
                total[1] = total[1] + (im * rr - re * ri)

            x_inverse(total[0], total[1], m, at)
        start(m)
    for m, group in enumerate(TAIL_GROUPS, start=parts + 2):
        whole(m).wait_recv()
        for at, d in enumerate(group):
            correction = y_inverse(m, at)
            for a in range(q):
                cols = slice(a * n, (a + 1) * n)
                out_ref[d, :, cols] = vol_ref[d, :, cols] * correction[a * q : (a + 1) * q]
    for m in range(messages):
        whole(m).wait_send()
    each_tile(lambda at: main_copy(at).wait_send())
    if shares == 2:
        each_tile(lambda at: pass_copy(at).wait_send())

    @pl.when(me < middle)
    def _():
        row_copy(middle).wait_send()


def place(*refs):
    sources, targets, held, sems = refs[:2], refs[2:4], refs[4:6], refs[6]
    reads = [pltpu.make_async_copy(sources[i], held[i], sems.at[0, i]) for i in range(2)]
    writes = [pltpu.make_async_copy(held[i], targets[i], sems.at[1, i]) for i in range(2)]
    for copy in reads:
        copy.start()
    for read, write in zip(reads, writes):
        read.wait()
        write.start()
    for write in writes:
        write.wait()


def shards(volume, psf_spectra, background, measured):
    n = lax.axis_size("row")
    slices, q, length = volume.shape
    shares = 2 if lax.axis_size("vol") % 2 == 0 else 1
    consts = tables(n, q)
    args = (volume, psf_spectra, background, measured, *consts)
    sizes = lambda groups: [2 * len(group) for group in groups]
    counts = sizes(HEAD_GROUPS) + [2, 2] + sizes(TAIL_GROUPS)
    in_vmem = pl.BlockSpec(memory_space=pltpu.VMEM)
    in_hbm = pl.BlockSpec(memory_space=pltpu.HBM)
    exchanged = [pltpu.VMEM((n, count, n), F32) for count in counts]
    tile = lambda *lead: pltpu.VMEM((*lead, n, n), F32)
    shapes = (
        jax.ShapeDtypeStruct(volume.shape, F32),
        jax.ShapeDtypeStruct(measured.shape, F32),
    )
    results = pl.pallas_call(
        functools.partial(kernel, n, q, slices, counts, shares),
        out_shape=shapes,
        in_specs=[in_hbm] * len(args),
        out_specs=(in_vmem, in_vmem),
        scratch_shapes=[pltpu.VMEM(arg.shape, arg.dtype) for arg in args]
        + exchanged
        + exchanged
        + [
            tile(2 * slices),
            tile(2 * slices),
            tile(2 * slices),
            tile(),
            tile(),
            tile(),
            tile(2 * slices),
            tile(2 * slices),
            tile(2, slices),
            tile(2),
            tile(2),
            pltpu.SemaphoreType.DMA((len(args),)),
            pltpu.SemaphoreType.DMA((len(counts),)),
            pltpu.SemaphoreType.DMA((len(counts),)),
            pltpu.SemaphoreType.DMA((2, 2 * slices)),
            pltpu.SemaphoreType.DMA((2, 2 * slices)),
            pltpu.SemaphoreType.DMA((2,)),
            pltpu.SemaphoreType.REGULAR,
            pltpu.SemaphoreType.REGULAR,
            pltpu.SemaphoreType.REGULAR,
        ],
        compiler_params=pltpu.CompilerParams(
            collective_id=0, has_side_effects=True, vmem_limit_bytes=60 * 1024 * 1024
        ),
    )(*args)
    return pl.pallas_call(
        place,
        out_shape=shapes,
        in_specs=[in_hbm] * 2,
        out_specs=(in_hbm, in_hbm),
        scratch_shapes=[pltpu.VMEM(shape.shape, F32) for shape in shapes]
        + [pltpu.SemaphoreType.DMA((2, 2))],
        compiler_params=pltpu.CompilerParams(vmem_limit_bytes=60 * 1024 * 1024),
    )(*results)


def solution(mesh):
    in_specs = (
        P("vol", "row", None),
        P(None, None, "row", None),
        P("row", None),
        P(("vol", "row"), None),
    )
    out_specs = (P("vol", "row", None), P(("vol", "row"), None))
    return jax.shard_map(shards, mesh=mesh, in_specs=in_specs, out_specs=out_specs, check_vma=False)
```

```python
import functools

import jax
import jax.numpy as jnp
import ml_dtypes
import numpy as np
from jax import lax
from jax.experimental import pallas as pl
from jax.experimental.pallas import tpu as pltpu
from jax.sharding import PartitionSpec as P

FLOOR = 0.5
F32 = jnp.float32
BF16 = jnp.bfloat16
NN = (((1,), (0,)), ((), ()))
NT = (((1,), (1,)), ((), ()))
HEAD_GROUPS = ((0, 1, 2),)
TAIL_GROUPS = ((0,), (1, 2))


def split_np(table):
    hi = table.astype(np.float32).astype(ml_dtypes.bfloat16)
    lo = (table - hi.astype(np.float64)).astype(np.float32).astype(ml_dtypes.bfloat16)
    return np.stack([hi, lo])


def tables(n, q):
    length = n * q
    half = q // 2
    lanes = half * q
    big = np.exp(-2j * np.pi * np.outer(np.arange(n), np.arange(n)) / n)
    small = np.exp(-2j * np.pi * np.outer(np.arange(q), np.arange(q)) / q)
    big_stack = np.block([[big.real, -big.imag], [big.imag, big.real]])
    spread = np.kron(small[: half + 1], np.eye(q))
    ycols = np.concatenate([spread.real, spread.imag], axis=0)
    yrows = np.zeros((q * q, 2, 2 * lanes))
    yrows[:, 0, : (half + 1) * q] = spread.real.T
    yrows[:, 1, : (half + 1) * q] = spread.imag.T
    mixed = np.einsum("xk,ij->ixkj", small, np.eye(half)).reshape(lanes, q * half)
    xmix = np.block([[mixed.real, mixed.imag], [-mixed.imag, mixed.real]])
    twist = np.exp(-2j * np.pi * np.outer(np.arange(q), np.arange(n)) / length)
    ytw = np.repeat(twist[: half + 1], q, axis=0)
    ytwt = np.zeros((n, 2 * lanes), complex)
    ytwt[:, : (half + 1) * q] = ytw.T
    xtw = np.tile(twist.T, (1, half))
    pair = lambda z: np.stack([z.real, z.imag]).astype(np.float32)
    return (
        split_np(ycols),
        pair(ytw),
        split_np(big_stack),
        pair(xtw),
        split_np(xmix),
        pair(ytwt),
        split_np(yrows.reshape(q * q, 4 * lanes)),
    )


def split(value):
    hi = value.astype(BF16)
    return hi, (value - hi.astype(F32)).astype(BF16)


def dot(left, right, dims):
    return lax.dot_general(left, right, dimension_numbers=dims, preferred_element_type=F32)


def dot3(left, right, dims):
    return dot(left[0], right[0], dims) + dot(left[0], right[1], dims) + dot(left[1], right[0], dims)


def kernel(n, q, slices, counts, shares, *refs):
    ins, refs = refs[:11], refs[11:]
    out_ref, proj_ref = refs[:2]
    held, refs = refs[2:13], refs[13:]
    messages = len(counts)
    sends, recvs = refs[:messages], refs[messages : 2 * messages]
    (
        own_half, main_send, main_recv, row_send, row_self, row_recv, resp, resp_mix, spec, spec_mix, total,
        in_sems, send_sems, recv_sems, psf_sems, pass_sems, row_sems, late_sem, both_sem, pass_sem,
    ) = refs[2 * messages :]
    vol_ref, psf_ref, back_ref, meas_ref, ycol_ref, ytw_ref, big_ref, xtw_ref, xmix_ref, ytwt_ref, yrow_ref = held
    order = (1, 0, 4, 5, 6, 7, 8, 9, 10, 2, 3)
    parts = len(HEAD_GROUPS)
    half = q // 2
    middle = n // 2
    scale = 1.0 / (n * q * n * q)
    me = lax.axis_index("row")
    vol_id = lax.axis_index("vol")
    share = lax.rem(vol_id, shares)
    other_vol = vol_id + (1 - 2 * share)
    tiles = range(2 * slices)

    def owned(at, mine=True):
        owner = 0 if shares == 1 or at < 2 * slices * 2 // 3 else 1
        return (share == owner) if mine else (share != owner)

    row_iota = lax.broadcasted_iota(jnp.int32, (n, n), 0)
    lane_iota = lax.broadcasted_iota(jnp.int32, (n, n), 1)

    def fetch(i):
        return pltpu.make_async_copy(ins[i], held[i], in_sems.at[i])

    for i in order:
        fetch(i).start()

    def device(dst, vol=None):
        return (vol_id if vol is None else vol, dst)

    def tell(sem, dst, vol=None):
        pl.semaphore_signal(sem, inc=1, device_id=device(dst, vol), device_id_type=pl.DeviceIdType.MESH)

    barrier = pltpu.get_barrier_semaphore()

    def peer(step):
        return jnp.bitwise_and(me + step, n - 1)

    @pl.when(me < 2)
    def _():
        tell(barrier, 1 - me)

    if shares == 2:

        @pl.when(me == 2)
        def _():
            tell(barrier, me, other_vol)

    @pl.when(me >= 2)
    def _():
        @pl.loop(1, n, unroll=8)
        def _(step):
            tell(barrier, peer(step))

    def copy_to(m, dst):
        return pltpu.make_async_remote_copy(
            src_ref=sends[m].at[dst],
            dst_ref=recvs[m].at[me],
            send_sem=send_sems.at[m],
            recv_sem=recv_sems.at[m],
            device_id=device(dst),
            device_id_type=pl.DeviceIdType.MESH,
        )

    def start(m):
        @pl.loop(1, n, unroll=8)
        def _(step):
            copy_to(m, peer(step)).start()

        recvs[m][me] = sends[m][me]

    def whole(m):
        return pltpu.make_async_remote_copy(
            src_ref=sends[m].at[pl.ds(0, n - 1)],
            dst_ref=recvs[m].at[pl.ds(0, n - 1)],
            send_sem=send_sems.at[m],
            recv_sem=recv_sems.at[m],
            device_id=device(peer(1)),
            device_id_type=pl.DeviceIdType.MESH,
        )

    def main_copy(at):
        return pltpu.make_async_remote_copy(
            src_ref=main_send.at[at],
            dst_ref=main_recv.at[at],
            send_sem=psf_sems.at[0, at],
            recv_sem=psf_sems.at[1, at],
            device_id=device(n - 1 - me),
            device_id_type=pl.DeviceIdType.MESH,
        )

    def pass_copy(at):
        return pltpu.make_async_remote_copy(
            src_ref=main_recv.at[at],
            dst_ref=main_recv.at[at],
            send_sem=pass_sems.at[0, at],
            recv_sem=pass_sems.at[1, at],
            device_id=device(me, other_vol),
            device_id_type=pl.DeviceIdType.MESH,
        )

    def each_tile(act, mine=True):
        for at in tiles:
            pl.when(owned(at, mine))(functools.partial(act, at))

    def row_copy(dst):
        return pltpu.make_async_remote_copy(
            src_ref=row_send,
            dst_ref=row_recv,
            send_sem=row_sems.at[0],
            recv_sem=row_sems.at[1],
            device_id=device(dst),
            device_id_type=pl.DeviceIdType.MESH,
        )

    def table(ref):
        return ref[0], ref[1]

    def y_forward(field, m, at):
        mixed = dot3(table(ycol_ref), split(field), NN)
        kept = (half + 1) * q
        re, im = mixed[:kept], mixed[kept:]
        wr, wi = ytw_ref[0], ytw_ref[1]
        turned = jnp.concatenate([re * wr - im * wi, re * wi + im * wr], axis=1)
        both = jnp.concatenate([turned[: half * q], turned[half * q :], turned[q : half * q]], axis=0)
        got = dot3(table(big_ref), split(both), NT)
        lanes = half * q
        re = jnp.concatenate([got[:middle, lanes:], got[middle:n, :lanes]], axis=0)
        im = jnp.concatenate([got[n : n + middle, lanes:], got[n + middle :, :lanes]], axis=0)
        im = jnp.where((row_iota == middle) & (lane_iota < q), got[0:1, :lanes], im)
        sends[m][:, 2 * at, :] = re
        sends[m][:, 2 * at + 1, :] = im

    def x_forward(re, im):
        got = dot3(table(big_ref), split(jnp.concatenate([re, im], axis=0)), NN)
        re, im = got[:n], got[n:]
        wr, wi = xtw_ref[0], xtw_ref[1]
        turned = jnp.concatenate([re * wr - im * wi, re * wi + im * wr], axis=1)
        out = dot3(split(turned), table(xmix_ref), NN)
        return out[:, :n], out[:, n:]

    def conjugates(fields):
        re_sum = im_sum = jnp.zeros((n, n), F32)
        for d, (re, im) in enumerate(fields):
            mine = (lane_iota >= d * q) & (lane_iota < (d + 1) * q)
            if d:
                re, im = pltpu.roll(re, d * q, 1), pltpu.roll(im, d * q, 1)
            re_sum = jnp.where(mine, re, re_sum)
            im_sum = jnp.where(mine, -im, im_sum)
        return re_sum, im_sum

    def x_forward_both(re, im, fields):
        re_conj, im_conj = conjugates(fields)
        fields = jnp.concatenate(
            [jnp.concatenate([re, re_conj], axis=1), jnp.concatenate([im, im_conj], axis=1)], axis=0
        )
        got = dot3(table(big_ref), split(fields), NN)
        wr, wi = xtw_ref[0], xtw_ref[1]
        turned = []
        for at in range(2):
            re, im = got[:n, at * n : (at + 1) * n], got[n:, at * n : (at + 1) * n]
            turned.append(jnp.concatenate([re * wr - im * wi, re * wi + im * wr], axis=1))
        out = dot3(split(jnp.concatenate(turned, axis=0)), table(xmix_ref), NN)
        return (out[:n, :n], out[:n, n:]), (out[n:, :n], out[n:, n:])

    def spectrum(d, m, at, sources):
        def field(m, at):
            return recvs[m][:, 2 * at, :], recvs[m][:, 2 * at + 1, :]

        if not sources:
            spec[0, d], spec[1, d] = x_forward(*field(m, at))
            return

        @pl.when(me != middle)
        def _():
            spec[0, d], spec[1, d] = x_forward(*field(m, at))

        @pl.when(me == middle)
        def _():
            plain, conj = x_forward_both(*field(m, at), [field(*source) for source in sources])
            spec[0, d], spec[1, d] = plain
            spec_mix[0], spec_mix[1] = conj

    def x_inverse(re, im, m, at):
        mixed = dot3(split(jnp.concatenate([re, im], axis=1)), table(xmix_ref), NT)
        wr, wi = xtw_ref[0], xtw_ref[1]
        re, im = mixed[:, :n], mixed[:, n:]
        swapped = jnp.concatenate([im * wr - re * wi, re * wr + im * wi], axis=0)
        got = dot3(table(big_ref), split(swapped), NN)
        sends[m][:, 2 * at, :] = got[n:]
        sends[m][:, 2 * at + 1, :] = got[:n]

    def y_inverse(m, at):
        re, im = recvs[m][:, 2 * at, :], recvs[m][:, 2 * at + 1, :]
        first = lane_iota < q
        upper = first & (row_iota < middle)
        zero_row = first & (row_iota == 0)
        mid_row = first & (row_iota == middle)
        re_low = jnp.where(upper, 0.0, re)
        re_low = jnp.where(mid_row, 0.5 * re, re_low)
        re_low = jnp.where(zero_row, 0.5 * im[middle : middle + 1], re_low)
        im_low = jnp.where(upper | mid_row, 0.0, im)
        re_high, im_high = jnp.where(upper, re, 0.0), jnp.where(upper, im, 0.0)
        swapped = jnp.concatenate(
            [
                jnp.concatenate([im_low, im_high], axis=1),
                jnp.concatenate([re_low, re_high], axis=1),
            ],
            axis=0,
        )
        got = dot3(table(big_ref), split(swapped), NN)
        im, re = got[:n], got[n:]
        wr, wi = ytwt_ref[0], ytwt_ref[1]
        turned = jnp.concatenate([re * wr + im * wi, im * wr - re * wi], axis=1)
        return dot3(table(yrow_ref), split(turned), NT) * (2.0 * scale)

    fetch(1).wait()
    reverse = jnp.where((row_iota + lane_iota == n) | (row_iota + lane_iota == 0), 1.0, 0.0).astype(BF16)
    same_block = row_iota // half == lane_iota // half
    slot_sum = row_iota % half + lane_iota % half
    slot_flip = jnp.where(same_block & ((slot_sum == half) | (slot_sum == 0)), 1.0, 0.0).astype(BF16)

    def blocks(field, backwards):
        places = range(q - 1, -1, -1) if backwards else range(q)
        return jnp.concatenate([field[:, k * n : (k + 1) * n] for k in places], axis=0)

    def mend(field):
        return jnp.where(row_iota == 0, pltpu.roll(field, half, 1), field)

    sub_iota = lax.broadcasted_iota(jnp.int32, (half, n * q), 0)
    rows = []
    for part in range(2):
        for d in range(slices):
            at = part * slices + d
            both = psf_ref[part, d].astype(F32)
            low, high = both[:half], both[half:]
            rows.append(low[0:1])
            own = jnp.where((sub_iota == 0) & (me < middle), high, low)
            own_half[at] = 0.5 * blocks(own, False).T

    def prepare(at):
        high = psf_ref[at // slices, at % slices].astype(F32)[half:]
        turned = dot(reverse, blocks(high, True).astype(BF16), NT)
        turned = dot(turned.astype(BF16), slot_flip, NN)
        main_send[at] = (0.5 if at < slices else -0.5) * mend(turned)

    each_tile(prepare)
    packed = jnp.concatenate(rows + [jnp.zeros((half - 2 * slices, n * q), F32)], axis=0)
    turned = mend(dot(reverse, blocks(packed, True).astype(BF16), NT))
    mine = jnp.where(lane_iota % half < slices, 0.5, -0.5) * turned
    row_self[...] = mine
    row_send[...] = jnp.where(me == 0, mine + 0.5 * blocks(packed, False).T, mine)

    @pl.when(me == 2)
    def _():
        pl.semaphore_wait(barrier, n - 4 + shares)

    @pl.when(me > 2)
    def _():
        pl.semaphore_wait(barrier, n - 3)

    @pl.when(me < 2)
    def _():
        pl.semaphore_wait(barrier, n - 1)

    @pl.when(me == 1)
    def _():
        @pl.loop(2, n, unroll=6)
        def _(dst):
            tell(late_sem, dst)

    @pl.when(me >= n - 2)
    def _():
        pl.semaphore_wait(late_sem, 1)

    each_tile(lambda at: main_copy(at).start())

    @pl.when(me == 0)
    def _():
        row_copy(middle).start()

    @pl.when((me > 0) & (me < middle))
    def _():
        row_copy(n - me).start()

    for i in (0, 4, 5, 6):
        fetch(i).wait()
    for m, group in enumerate(HEAD_GROUPS):
        for at, d in enumerate(group):
            y_forward(
                jnp.concatenate([vol_ref[d, :, a * n : (a + 1) * n] for a in range(q)], axis=0), m, at
            )

    for m in range(parts):

        @pl.when(me >= 2)
        def _():
            @pl.loop(1, n - 2, unroll=5)
            def _(step):
                place = me + step
                copy_to(m, jnp.where(place >= n, place - (n - 2), place)).start()

        @pl.when(me < 2)
        def _():
            @pl.loop(1, n, unroll=8)
            def _(step):
                copy_to(m, peer(step)).start()

        recvs[m][me] = sends[m][me]

    @pl.when((me >= 2) & (me < n - 2))
    def _():
        pl.semaphore_wait(late_sem, 1)

    if shares == 2:

        @pl.when(me == 2)
        def _():
            tell(both_sem, me, other_vol)
            pl.semaphore_wait(both_sem, 1)

            @pl.loop(1, n, unroll=8)
            def _(step):
                tell(pass_sem, peer(step))

    @pl.when(me >= 2)
    def _():
        for dst in range(2):
            for m in range(parts):
                copy_to(m, dst).start()

    if shares == 2:

        @pl.when(me != 2)
        def _():
            pl.semaphore_wait(pass_sem, 1)

    def hand_on(at):
        main_copy(at).wait_recv()
        if shares == 2:
            pass_copy(at).start()

    each_tile(hand_on)
    for i in (7, 8):
        fetch(i).wait()

    heads = [(m, at) for m, group in enumerate(HEAD_GROUPS) for at in range(len(group))]

    def forward_group(m, group):
        whole(m).wait_recv()
        last = m == parts - 1
        for at, d in enumerate(group):
            spectrum(d, m, at, heads if last and at == 0 else ())

    forward_group(0, HEAD_GROUPS[0])
    if shares == 2:
        each_tile(lambda at: pass_copy(at).wait_recv(), mine=False)
    slot_zero = lane_iota % half == 0
    for at in range(2 * slices):
        resp[at] = own_half[at] + main_recv[at]

    def spread(field, at):
        return pltpu.roll(field, n - at, 1) if at else field

    @pl.when(me >= middle)
    def _():
        row_copy(middle).wait_recv()
        other = jnp.where(me == middle, row_self[...], row_recv[...])
        for at in range(2 * slices):
            resp[at] = jnp.where(slot_zero, own_half[at] + spread(other, at), resp[at])

    @pl.when(me == middle)
    def _():
        for at in range(2 * slices):
            edge = spread(row_recv[...], at)
            here = resp[at]
            resp[at] = jnp.where(slot_zero, 0.5 * (here + edge), here)
            resp_mix[at] = jnp.where(slot_zero, 0.5 * (here - edge), 0.0)

    for m, group in enumerate(HEAD_GROUPS[1:], start=1):
        forward_group(m, group)

    sum_re = sum_im = jnp.zeros((n, n), F32)
    for d in range(slices):
        re, im = spec[0, d], spec[1, d]
        rr, ri = resp[d], resp[slices + d]
        sum_re = sum_re + (re * rr - im * ri)
        sum_im = sum_im + (re * ri + im * rr)
    total[0] = sum_re
    total[1] = sum_im

    @pl.when(me == middle)
    def _():
        sum_re, sum_im = total[0], total[1]
        for d in range(slices):
            re, im = spread(spec_mix[0], d), spread(spec_mix[1], d)
            rr, ri = resp_mix[d], resp_mix[slices + d]
            sum_re = sum_re + (re * rr - im * ri)
            sum_im = sum_im + (re * ri + im * rr)
        total[0] = sum_re
        total[1] = sum_im

    x_inverse(total[0], total[1], parts, 0)
    start(parts)
    for i in (9, 10, 2, 3):
        fetch(i).wait()
    whole(parts).wait_recv()
    projection = y_inverse(parts, 0)
    quotient = []
    for a in range(q):
        cols = slice(a * n, (a + 1) * n)
        piece = projection[a * q : (a + 1) * q]
        proj_ref[:, cols] = piece
        quotient.append(meas_ref[:, cols] / jnp.maximum(piece + back_ref[:, cols], FLOOR))

    y_forward(jnp.concatenate(quotient, axis=0), parts + 1, 0)
    start(parts + 1)
    whole(parts + 1).wait_recv()
    spectrum(0, parts + 1, 0, [(parts + 1, 0)])

    for m, group in enumerate(TAIL_GROUPS, start=parts + 2):
        for at, d in enumerate(group):
            re, im = spec[0, 0], spec[1, 0]
            rr, ri = resp[d], resp[slices + d]
            total[0] = re * rr + im * ri
            total[1] = im * rr - re * ri

            @pl.when(me == middle)
            def _():
                re, im = spec_mix[0], spec_mix[1]
                rr, ri = resp_mix[d], resp_mix[slices + d]
                total[0] = total[0] + (re * rr + im * ri)
                total[1] = total[1] + (im * rr - re * ri)

            x_inverse(total[0], total[1], m, at)
        start(m)
    for m, group in enumerate(TAIL_GROUPS, start=parts + 2):
        whole(m).wait_recv()
        for at, d in enumerate(group):
            correction = y_inverse(m, at)
            for a in range(q):
                cols = slice(a * n, (a + 1) * n)
                out_ref[d, :, cols] = vol_ref[d, :, cols] * correction[a * q : (a + 1) * q]
    for m in range(messages):
        whole(m).wait_send()
    each_tile(lambda at: main_copy(at).wait_send())
    if shares == 2:
        each_tile(lambda at: pass_copy(at).wait_send())

    @pl.when(me < middle)
    def _():
        row_copy(middle).wait_send()


def place(*refs):
    sources, targets, held, sems = refs[:2], refs[2:4], refs[4:6], refs[6]
    reads = [pltpu.make_async_copy(sources[i], held[i], sems.at[0, i]) for i in range(2)]
    writes = [pltpu.make_async_copy(held[i], targets[i], sems.at[1, i]) for i in range(2)]
    for copy in reads:
        copy.start()
    for read, write in zip(reads, writes):
        read.wait()
        write.start()
    for write in writes:
        write.wait()


def shards(volume, psf_spectra, background, measured):
    n = lax.axis_size("row")
    slices, q, length = volume.shape
    shares = 2 if lax.axis_size("vol") % 2 == 0 else 1
    consts = tables(n, q)
    args = (volume, psf_spectra, background, measured, *consts)
    sizes = lambda groups: [2 * len(group) for group in groups]
    counts = sizes(HEAD_GROUPS) + [2, 2] + sizes(TAIL_GROUPS)
    in_vmem = pl.BlockSpec(memory_space=pltpu.VMEM)
    in_hbm = pl.BlockSpec(memory_space=pltpu.HBM)
    exchanged = [pltpu.VMEM((n, count, n), F32) for count in counts]
    tile = lambda *lead: pltpu.VMEM((*lead, n, n), F32)
    shapes = (
        jax.ShapeDtypeStruct(volume.shape, F32),
        jax.ShapeDtypeStruct(measured.shape, F32),
    )
    results = pl.pallas_call(
        functools.partial(kernel, n, q, slices, counts, shares),
        out_shape=shapes,
        in_specs=[in_hbm] * len(args),
        out_specs=(in_vmem, in_vmem),
        scratch_shapes=[pltpu.VMEM(arg.shape, arg.dtype) for arg in args]
        + exchanged
        + exchanged
        + [
            tile(2 * slices),
            tile(2 * slices),
            tile(2 * slices),
            tile(),
            tile(),
            tile(),
            tile(2 * slices),
            tile(2 * slices),
            tile(2, slices),
            tile(2),
            tile(2),
            pltpu.SemaphoreType.DMA((len(args),)),
            pltpu.SemaphoreType.DMA((len(counts),)),
            pltpu.SemaphoreType.DMA((len(counts),)),
            pltpu.SemaphoreType.DMA((2, 2 * slices)),
            pltpu.SemaphoreType.DMA((2, 2 * slices)),
            pltpu.SemaphoreType.DMA((2,)),
            pltpu.SemaphoreType.REGULAR,
            pltpu.SemaphoreType.REGULAR,
            pltpu.SemaphoreType.REGULAR,
        ],
        compiler_params=pltpu.CompilerParams(
            collective_id=0, has_side_effects=True, vmem_limit_bytes=60 * 1024 * 1024
        ),
    )(*args)
    return pl.pallas_call(
        place,
        out_shape=shapes,
        in_specs=[in_hbm] * 2,
        out_specs=(in_hbm, in_hbm),
        scratch_shapes=[pltpu.VMEM(shape.shape, F32) for shape in shapes]
        + [pltpu.SemaphoreType.DMA((2, 2))],
        compiler_params=pltpu.CompilerParams(vmem_limit_bytes=60 * 1024 * 1024),
    )(*results)


def solution(mesh):
    in_specs = (
        P("vol", "row", None),
        P(None, None, "row", None),
        P("row", None),
        P(("vol", "row"), None),
    )
    out_specs = (P("vol", "row", None), P(("vol", "row"), None))
    return jax.shard_map(shards, mesh=mesh, in_specs=in_specs, out_specs=out_specs, check_vma=False)
```
